128 devices in a mesh: seg: 32 (over y, x, core), col: 4 (over z).
Axes of the slice: x: 4, y: 4, z: 4, core: 2. Of those that a mesh axis runs over, the one named last changes fastest.
Arguments:
- diagonal: float32 [128, 512, 512], P('seg', None, 'col'), as said below
- lower: float32 [128, 512, 512], P('seg'), as said below
- right_side: float32 [128, 512, 512], P('seg', None, 'col'), may hold values from -0.375 to 0.375
Outputs:
- solution: float32 [128, 512, 512], P('seg', None, 'col')
The draws below stay inside these ranges and needn't reach their ends.
Inputs may be any that keep to these rules, and one draw needn't show every extreme that they name: Every diagonal block is symmetric, and with lower it makes A symmetric positive definite. `lower`: with diagonal it makes A symmetric positive definite.
All inputs are finite; a program needn't handle non-finite values.
Results may differ from the reference program's by a relative error of at most 0.0003.
Values sent between devices are 32-bit elements; how exact they have to be, the bound alone decides.
A program may use at most 192 MiB of HBM per device.

```python
import math
import jax
import jax.numpy as jnp
from jax import lax

B = 512
K = 4
NRHS = 512
NB = 128


def chain_parts(key):
    base_key = jax.random.fold_in(key, 7)
    first_key, second_key, rate_key = jax.random.split(base_key, 3)
    noise_shape = (NB, B, B)
    first_noise = jax.random.normal(first_key, noise_shape, jnp.float32)
    second_noise = jax.random.normal(second_key, noise_shape, jnp.float32)
    decay_rates = jax.random.uniform(rate_key, (NB,), jnp.float32, 0.0, 0.1)
    carry_ratio = 1.0 - decay_rates / K
    identity = jnp.eye(B, dtype=jnp.float32)
    noise_scale = 0.3 / math.sqrt(B)
    upper_part = identity + noise_scale * first_noise
    lower_part = carry_ratio[:, None, None] * (identity + noise_scale * second_noise)
    return (upper_part, lower_part)


def draw_diagonal(key, part):
    upper_part, lower_part = chain_parts(key)
    gram_sum = jnp.einsum('nki,nkj->nij', upper_part, upper_part, precision=lax.Precision.HIGHEST)
    gram_sum = gram_sum + jnp.einsum('nki,nkj->nij', lower_part, lower_part, precision=lax.Precision.HIGHEST)
    gram_sum = 0.5 * (gram_sum + jnp.swapaxes(gram_sum, 1, 2))
    return gram_sum + 0.05 / (K * K) * jnp.eye(B, dtype=jnp.float32)


def draw_lower(key, part):
    upper_part, lower_part = chain_parts(key)
    shifted = jnp.roll(lower_part, 1, axis=0)
    return -jnp.einsum('nki,nkj->nij', upper_part, shifted, precision=lax.Precision.HIGHEST)


def shard_levels(rng, extent, shards, low, top_value):
    loudness = 1.0
    for position, shards_of in shards:
        steps = jax.random.uniform(jax.random.fold_in(jax.random.fold_in(rng, 6), position), (shards_of,), jnp.float32, low / len(shards), top_value / len(shards))
        loudness = loudness * jnp.repeat(jnp.exp(steps), extent[position] // shards_of).reshape((-1,) + (1,) * (len(extent) - 1 - position))
    return loudness


def centred(rng, shape, spread, limit, pieces=(), held_as=jnp.bfloat16):
    values = spread * jax.random.normal(rng, shape, jnp.float32)
    if pieces:
        values = values * shard_levels(rng, shape, pieces, -0.22, 0.18)
    return jnp.clip(values, -limit, limit).astype(held_as)


def setup_inputs(seed: int = 0) -> dict:
    streams_of = jax.random.split(jax.random.key(seed), 4)
    return {
        "diagonal": draw_diagonal(jax.random.fold_in(streams_of[3], 71), 0),
        "lower": draw_lower(jax.random.fold_in(streams_of[3], 71), 0),
        "right_side": centred(streams_of[2], (NB, B, NRHS), (1.0 / (K * K)), 0.375, ((0, 32), (2, 4)), jnp.float32),
    }


def matmul(left_hand, right_hand):
    return jnp.dot(left_hand.astype(jnp.float32), right_hand.astype(jnp.float32), precision=lax.Precision.HIGHEST, preferred_element_type=jnp.float32)

def chol_solve(factor, right_hand):
    halfway = lax.linalg.triangular_solve(factor, right_hand, left_side=True, lower=True)
    return lax.linalg.triangular_solve(factor, halfway, left_side=True, lower=True, transpose_a=True)

def reference(diagonal, lower, right_side):
    blocks = diagonal.shape[0]
    left_mask = (jnp.arange(blocks) > 0).astype(jnp.float32)[:, None, None]
    couple = lower * left_mask
    identity = jnp.eye(B, dtype=jnp.float32)

    def forward(state, inputs):
        factor, previous = state
        diag_block, coupling, rhs_block = inputs
        schur = diag_block - matmul(coupling, chol_solve(factor, coupling.T))
        new_factor = jnp.linalg.cholesky(schur)
        advanced = rhs_block - matmul(coupling, chol_solve(factor, previous))
        return ((new_factor, advanced), (new_factor, advanced))
    start_state = (identity, jnp.zeros((B, NRHS), jnp.float32))
    final_state, (factors, advanced) = lax.scan(forward, start_state, (diagonal, couple, right_side))
    next_links = jnp.concatenate([couple[1:], jnp.zeros((1, B, B), jnp.float32)], axis=0)

    def backward(later_block, inputs):
        factor, advanced_block, coupling = inputs
        solved = chol_solve(factor, advanced_block - matmul(coupling.T, later_block))
        return (solved, solved)
    last_state, solution = lax.scan(backward, jnp.zeros((B, NRHS), jnp.float32), (factors, advanced, next_links), reverse=True)
    return solution
```

```python
import jax
import jax.numpy as jnp
from jax import lax
from jax.experimental import pallas as pl
from jax.experimental.pallas import tpu as pltpu
from jax.sharding import PartitionSpec as P


def passed_along(shard, axis, by):
    size = lax.axis_size(axis)
    pairs = [(i, i + by) for i in range(size) if 0 <= i + by < size]
    return lax.ppermute(shard, axis, pairs)


def matmul(left_hand, right_hand):
    return jnp.dot(
        left_hand, right_hand, precision=lax.Precision.HIGHEST, preferred_element_type=jnp.float32
    )


W = 16

def invert_panel(lanes, block, k):
    first = W * k
    tiles = W // 8
    rows = jnp.concatenate(block[tiles * k: tiles * (k + 1)], axis=0)
    cols = [jnp.broadcast_to(rows[:, first + p: first + p + 1], (W, 128)) for p in range(W)]
    others = [i for i in range(16) if not tiles * k <= i < tiles * (k + 1)]
    wide = {i: [jnp.broadcast_to(block[i][:, first + p: first + p + 1], (8, 128)) for p in range(W)] for i in others}
    inside = (lanes >= first) & (lanes < first + W)
    sub16 = lax.broadcasted_iota(jnp.int32, (W, 128), 0)
    lane16 = lax.broadcasted_iota(jnp.int32, (W, 128), 1)
    rows = jnp.where((lane16 >= first) & (lane16 < first + W), (lane16 - first == sub16).astype(jnp.float32), rows)
    for p in range(W):
        pivot = 1.0 / cols[p][p:p + 1, :]
        here = sub16 == p
        scaled = rows[p:p + 1, :] * pivot
        rows = jnp.where(here, scaled, rows - cols[p] * scaled)
        for j in range(p + 1, W):
            scaled_j = cols[j][p:p + 1, :] * pivot
            cols[j] = jnp.where(here, scaled_j, cols[j] - cols[p] * scaled_j)
    out = [None] * 16
    for i in range(tiles):
        out[tiles * k + i] = rows[8 * i: 8 * i + 8]
    for i in others:
        acc = jnp.where(inside, 0.0, block[i])
        for p in range(W):
            acc = acc - wide[i][p] * rows[p:p + 1, :]
        out[i] = acc
    return out

def invert128(block):
    lanes = lax.broadcasted_iota(jnp.int32, (8, 128), 1)
    tiles = [block[8 * i: 8 * i + 8] for i in range(16)]
    for k in range(128 // W):
        tiles = invert_panel(lanes, tiles, k)
    return jnp.concatenate(tiles, axis=0)

def k512(x, o):
    o[...] = x[...]
    def step(j, c):
        s = pl.ds(pl.multiple_of(j * 128, 128), 128)
        w = invert128(o[s, s])
        row = o[s, :]
        t = matmul(w, row)
        col = o[:, s]
        rowid = lax.broadcasted_iota(jnp.int32, (512, 1), 0) // 128
        u = jnp.where(rowid == j, 0.0, col)
        o[:, s] = jnp.zeros((512, 128), jnp.float32)
        lane = lax.broadcasted_iota(jnp.int32, (1, 512), 1) // 128
        wt = jnp.concatenate([w] * 4, axis=1)
        t = jnp.where(lane == j, wt, t)
        o[...] = o[...] - matmul(u, t)
        o[s, :] = t
        return c
    lax.fori_loop(0, 4, step, 0)


def invert_spd(matrix):
    return pl.pallas_call(
        k512,
        out_shape=jax.ShapeDtypeStruct(matrix.shape, jnp.float32),
        in_specs=[pl.BlockSpec(memory_space=pltpu.VMEM)],
        out_specs=pl.BlockSpec(memory_space=pltpu.VMEM),
    )(matrix)


def backward_sweep(inverses, next_links, advanced):

    def backward(later_block, inputs):
        inverse, advanced_block, coupling = inputs
        solved = matmul(inverse, advanced_block - matmul(coupling.T, later_block))
        return (solved, solved)

    last_state, solved = lax.scan(
        backward, jnp.zeros_like(advanced[0]), (inverses, advanced, next_links), reverse=True
    )
    return solved


def on_device(diagonal, lower, right_side):
    blocks = lower.shape[0]
    block_size = lower.shape[1]
    col_share = diagonal.shape[2]
    rhs_cols = right_side.shape[2]
    interior = blocks - 1
    offset = lax.axis_index("col") * col_share
    has_left = (lax.axis_index("seg") > 0).astype(jnp.float32)
    left_block = lower[0] * has_left
    sep_block = lower[blocks - 1]
    identity = jnp.eye(block_size, dtype=jnp.float32)
    left_mask = (jnp.arange(interior) > 0).astype(jnp.float32)[:, None, None]
    couple = lower[:interior] * left_mask
    next_links = jnp.concatenate(
        [couple[1:], jnp.zeros((1, block_size, block_size), jnp.float32)], axis=0
    )
    left_cols = lax.dynamic_slice_in_dim(left_block, offset, col_share, 1)
    right_cols = lax.dynamic_slice_in_dim(sep_block, offset, col_share, 0).T
    empty_cols = jnp.zeros((interior, block_size, col_share), jnp.float32)
    stacked = jnp.concatenate(
        [
            empty_cols.at[0].set(left_cols),
            empty_cols.at[interior - 1].set(right_cols),
            right_side[:interior],
        ],
        axis=2,
    )
    diag_items = diagonal[:interior]

    def forward(state, inputs):
        inverse, previous = state
        diag_block, coupling, rhs_block = inputs
        link_rows = lax.dynamic_slice_in_dim(coupling, offset, col_share, 0)
        partial_cols = diag_block - matmul(coupling, matmul(inverse, link_rows.T))
        schur = lax.all_gather(partial_cols, "col", axis=1, tiled=True)
        new_inverse = invert_spd(schur)
        advanced = rhs_block - matmul(coupling, matmul(inverse, previous))
        return ((new_inverse, advanced), (new_inverse, advanced))

    start_state = (identity, jnp.zeros((block_size, stacked.shape[2]), jnp.float32))
    final_state, (inverses, advanced) = lax.scan(
        forward, start_state, (diag_items, couple, stacked)
    )
    solved = backward_sweep(inverses, next_links, advanced)
    own_terms = matmul(sep_block, solved[interior - 1])
    next_terms = passed_along(matmul(left_block.T, solved[0]), "seg", -1)
    pivot_block = (
        diagonal[blocks - 1] - own_terms[:, col_share : 2 * col_share] - next_terms[:, :col_share]
    )
    sub_block = -own_terms[:, :col_share]
    super_block = -next_terms[:, col_share : 2 * col_share]
    reduced_rhs = (
        right_side[blocks - 1] - own_terms[:, 2 * col_share :] - next_terms[:, 2 * col_share :]
    )
    levels = (lax.axis_size("seg") - 1).bit_length()
    for level_bit in range(levels):
        stride = 1 << level_bit
        pivot_full, sub_full, super_full = (
            lax.all_gather(pivot_block, "col", axis=1, tiled=True),
            lax.all_gather(sub_block, "col", axis=1, tiled=True),
            lax.all_gather(super_block, "col", axis=1, tiled=True),
        )
        pivot_inverse = invert_spd(pivot_full)
        scaled = matmul(
            pivot_inverse, jnp.concatenate([sub_block, super_block, reduced_rhs], axis=1)
        )
        lower_terms = passed_along(scaled, "seg", stride)
        upper_terms = passed_along(scaled, "seg", -stride)
        narrow = sub_block.shape[1]
        new_sub = -matmul(sub_full, lower_terms[:, :narrow])
        new_super = -matmul(super_full, upper_terms[:, narrow : 2 * narrow])
        pivot_block = (
            pivot_block
            - matmul(sub_full, lower_terms[:, narrow : 2 * narrow])
            - matmul(super_full, upper_terms[:, :narrow])
        )
        reduced_rhs = (
            reduced_rhs
            - matmul(sub_full, lower_terms[:, 2 * narrow :])
            - matmul(super_full, upper_terms[:, 2 * narrow :])
        )
        sub_block, super_block = (new_sub, new_super)
    pivot_full = lax.all_gather(pivot_block, "col", axis=1, tiled=True)
    separator = matmul(invert_spd(pivot_full), reduced_rhs)
    left_sep = passed_along(separator, "seg", 1)
    correction = jnp.zeros((interior, block_size, rhs_cols), jnp.float32)
    correction = correction.at[0].add(matmul(left_block, left_sep))
    correction = correction.at[interior - 1].add(matmul(sep_block.T, separator))
    previous_inverses = jnp.concatenate([identity[None], inverses[:-1]], axis=0)

    def forward_only(previous, inputs):
        inverse, coupling, rhs_block = inputs
        advanced_block = rhs_block - matmul(coupling, matmul(inverse, previous))
        return (advanced_block, advanced_block)

    last_pushed, pushed = lax.scan(
        forward_only,
        jnp.zeros((block_size, rhs_cols), jnp.float32),
        (previous_inverses, couple, correction),
    )
    adjust = backward_sweep(inverses, next_links, pushed)
    interior_part = solved[:, :, 2 * col_share :] - adjust
    return jnp.concatenate([interior_part, separator[None]], axis=0)


def solution(mesh):
    in_specs = (P("seg", None, "col"), P("seg", None, None), P("seg", None, "col"))
    out_specs = P("seg", None, "col")
    return jax.shard_map(
        on_device, mesh=mesh, in_specs=in_specs, out_specs=out_specs, check_vma=False
    )
```

```python
import functools
import jax
import jax.numpy as jnp
from jax import lax
from jax.experimental import pallas as pl
from jax.experimental.pallas import tpu as pltpu
from jax.sharding import PartitionSpec as P

W = 16
BF = jnp.bfloat16
F32 = jnp.float32


def invert_panel(lanes, block, k):
    first = W * k
    tiles = W // 8
    rows = jnp.concatenate(block[tiles * k : tiles * (k + 1)], axis=0)
    cols = [jnp.broadcast_to(rows[:, first + p : first + p + 1], (W, 128)) for p in range(W)]
    others = [i for i in range(16) if not tiles * k <= i < tiles * (k + 1)]
    wide = {
        i: [jnp.broadcast_to(block[i][:, first + p : first + p + 1], (8, 128)) for p in range(W)]
        for i in others
    }
    inside = (lanes >= first) & (lanes < first + W)
    sub = lax.broadcasted_iota(jnp.int32, (W, 128), 0)
    lane = lax.broadcasted_iota(jnp.int32, (W, 128), 1) - first
    rows = jnp.where((lane >= 0) & (lane < W), (lane == sub).astype(F32), rows)
    for p in range(W):
        pivot = 1.0 / cols[p][p : p + 1, :]
        here = sub == p
        scaled = rows[p : p + 1, :] * pivot
        rows = jnp.where(here, scaled, rows - cols[p] * scaled)
        for j in range(p + 1, W):
            scaled_j = cols[j][p : p + 1, :] * pivot
            cols[j] = jnp.where(here, scaled_j, cols[j] - cols[p] * scaled_j)
    out = [None] * 16
    for i in range(tiles):
        out[tiles * k + i] = rows[8 * i : 8 * i + 8]
    for i in others:
        acc = jnp.where(inside, 0.0, block[i])
        for p in range(W):
            acc = acc - wide[i][p] * rows[p : p + 1, :]
        out[i] = acc
    return out


def invert128(block):
    lanes = lax.broadcasted_iota(jnp.int32, (8, 128), 1)
    tiles = [block[8 * i : 8 * i + 8] for i in range(16)]
    for k in range(128 // W):
        tiles = invert_panel(lanes, tiles, k)
    return jnp.concatenate(tiles, axis=0)


def pieces(x):
    high = x.astype(BF)
    rest = x - high.astype(F32)
    mid = rest.astype(BF)
    low = (rest - mid.astype(F32)).astype(BF)
    return high, mid, low


def left6(x):
    h, m, l = pieces(x)
    return jnp.concatenate([h, m, h, m, h, l], axis=1)


def right6(x):
    h, m, l = pieces(x)
    return jnp.concatenate([h, h, m, m, l, h], axis=0)


def dot(a, b):
    return jnp.dot(a, b, preferred_element_type=F32)


def at(i, size):
    return pl.ds(pl.multiple_of(i * size, size), size)


def reduce_rows(m, u6, n_tiles):
    def step(j, c):
        s = at(j, 128)
        w6 = left6(invert128(m[s, s]))
        rowid = lax.broadcasted_iota(jnp.int32, (512, 1), 0) // 128
        u6[...] = left6(jnp.where(rowid == j, 0.0, m[:, s]))

        def tile(i, c):
            n = at(i, 256)
            t = dot(w6, right6(m[s, n]))
            t6 = right6(t)
            m[:, n] = m[:, n] - dot(u6[...], t6)
            m[s, n] = t
            return c

        lax.fori_loop((j + 1) // 2, n_tiles, tile, 0)
        return c

    lax.fori_loop(0, 4, step, 0)


def schur(et, g3, m, base, outs):
    ll, lr, rr, rl_, rr_ = outs
    b_ll, b_rr, b_rl_, b_rr_ = base
    parts = pieces(m[:, 512:1792])
    for q in range(3):
        g3[q] = parts[q]

    def term(i, n, cols=256):
        e = left6(et[at(i, 256), :])
        c = pl.ds(pl.multiple_of(n * 256, 256), cols)
        h, mm, l = g3[0, :, c], g3[1, :, c], g3[2, :, c]
        return dot(e, jnp.concatenate([h, h, mm, mm, l, h], axis=0))

    def body(q, c):
        i, n = q // 2, q % 2
        r, k = at(i, 256), at(n, 256)
        ll[r, k] = b_ll(r, k) - term(i, n)
        lr[r, k] = -term(i, n + 2)
        rr[r, k] = b_rr(r, k) - term(i + 2, n + 2)
        return c

    lax.fori_loop(0, 4, body, 0)

    def rhs(i, c):
        r = at(i, 256)
        rl_[r, :] = b_rl_(r) - term(i, 4, 128)
        rr_[r, :] = b_rr_(r) - term(i + 2, 4, 128)
        return c

    lax.fori_loop(0, 2, rhs, 0)


def fill(m, et, f):
    m[:, 1536:1664] = f
    m[:, 1664:1792] = jnp.zeros((512, 128), F32)


def first_kernel(p, x1, x2, f, d, fd, g, gf, ll, lr, rr, rl_, rr_, m, u6, et, g3):
    m[:, 0:512] = p[...]
    m[:, 512:1024] = x1[...]
    et[0:512, :] = x1[...].T
    et[512:1024, :] = x2[...]
    m[:, 1024:1536] = x2[...].T
    fill(m, et, f[...])
    reduce_rows(m, u6, 7)
    g[...] = m[:, 512:1536]
    gf[...] = m[:, 1536:1664]
    zero = lambda r, k=None: 0.0
    schur(et, g3, m, (zero, lambda r, k: d[r, k], zero, lambda r: fd[r, :]), (ll, lr, rr, rl_, rr_))


def merge_kernel(bit, all_, alr, arr, arl, arr_, bll, blr, brr, brl, brr_,
                 g, gf, ll, lr, rr, rl_, rr_, m, u6, et, g3):
    def load(own, other):
        oll, olr, orr, orl, orr_ = own
        pll, plr, prr, prl, prr_ = other
        m[:, 0:512] = orr[...] + pll[...]
        et[0:512, :] = olr[...]
        m[:, 1024:1536] = plr[...]
        ll[...] = oll[...]
        rr[...] = prr[...]
        rl_[...] = orl[...]
        rr_[...] = prr_[...]
        fill(m, et, orr_[...] + prl[...])

    mine = (all_, alr, arr, arl, arr_)
    other = (bll, blr, brr, brl, brr_)

    @pl.when(bit[0] == 0)
    def _():
        load(mine, other)

    @pl.when(bit[0] != 0)
    def _():
        load(other, mine)

    m[:, 512:1024] = et[0:512, :].T
    et[512:1024, :] = m[:, 1024:1536].T
    reduce_rows(m, u6, 7)
    g[...] = m[:, 512:1536]
    gf[...] = m[:, 1536:1664]
    schur(et, g3, m,
          (lambda r, k: ll[r, k], lambda r, k: rr[r, k], lambda r: rl_[r, :], lambda r: rr_[r, :]),
          (ll, lr, rr, rl_, rr_))


def last_kernel(p, f, x, m, u6):
    m[:, 0:512] = p[...]
    m[:, 512:640] = f[...]
    m[:, 640:768] = jnp.zeros((512, 128), F32)
    reduce_rows(m, u6, 3)
    x[...] = m[:, 512:640]


def vm(n):
    return [pl.BlockSpec(memory_space=pltpu.VMEM)] * n


def shapes(*dims):
    return tuple(jax.ShapeDtypeStruct(d, F32) for d in dims)


SQ, TH = (512, 512), (512, 128)
STATE = (SQ, SQ, SQ, TH, TH)
PARAMS = pltpu.CompilerParams(vmem_limit_bytes=44 * 2**20)
COST = pl.CostEstimate(flops=18 * 10**9, bytes_accessed=2**24, transcendentals=0)
WORK = [
    pltpu.VMEM((512, 1792), F32),
    pltpu.VMEM((512, 768), BF),
    pltpu.VMEM((1024, 512), F32),
    pltpu.VMEM((3, 512, 1280), BF),
]


def eliminate(p, x1, x2, f, d, fd):
    out = pl.pallas_call(
        first_kernel, out_shape=shapes((512, 1024), TH, *STATE), in_specs=vm(6), out_specs=vm(7),
        scratch_shapes=WORK, compiler_params=PARAMS, cost_estimate=COST,
    )(p, x1, x2, f, d, fd)
    return out[:2], out[2:]


def merge(bit, mine, other):
    out = pl.pallas_call(
        merge_kernel, out_shape=shapes((512, 1024), TH, *STATE),
        in_specs=[pl.BlockSpec(memory_space=pltpu.SMEM)] + vm(10), out_specs=vm(7),
        scratch_shapes=WORK, compiler_params=PARAMS, cost_estimate=COST,
    )(bit, *mine, *other)
    return out[:2], out[2:]


def finish(p, f):
    return pl.pallas_call(
        last_kernel, out_shape=shapes(TH)[0], in_specs=vm(2), out_specs=vm(1)[0],
        scratch_shapes=[pltpu.VMEM((512, 768), F32), WORK[1]], compiler_params=PARAMS, cost_estimate=COST,
    )(p, f)


MESH_ID = pl.DeviceIdType.MESH


def partner_of(seg, level):
    if level == 0:
        return seg + 1 - 2 * lax.rem(seg, 2)
    core, x, y = lax.rem(seg, 2), lax.rem(lax.div(seg, 2), 4), lax.div(seg, 8)
    if level == 1:
        x = x + 1 - 2 * lax.rem(x, 2)
    if level == 2:
        x = 3 - x
    if level == 3:
        y = y + 1 - 2 * lax.rem(y, 2)
    if level == 4:
        y = 3 - y
    return (y * 4 + x) * 2 + core


def exchange_kernel(level, m, r, pm, pr, sx, rx, sz, rz, sd, rd):
    seg, col = lax.axis_index("seg"), lax.axis_index("col")
    core = lax.rem(seg, 2)
    sibling = partner_of(seg, 0)
    partner = partner_of(seg, level)
    barrier = pltpu.get_barrier_semaphore()
    peers = [(sibling, col)]
    if level > 0:
        peers += [(partner, col)] + [(seg, lax.rem(col + d, 4)) for d in (1, 2, 3)]
    for peer in peers:
        pl.semaphore_signal(barrier, inc=1, device_id=peer, device_id_type=MESH_ID)
    pl.semaphore_wait(barrier, len(peers))

    def copy(src, dst, s, d, peer):
        return pltpu.make_async_remote_copy(
            src_ref=src, dst_ref=dst, send_sem=s, recv_sem=d, device_id=peer, device_id_type=MESH_ID
        )

    if level == 0:
        copies = [
            copy(m, pm, sx.at[0], rx.at[0], (partner, col)),
            copy(r, pr, sx.at[1], rx.at[1], (partner, col)),
        ]
        for c in copies:
            c.start()
        for c in copies:
            c.wait()
        return
    rows = 1536 // 8 // CHUNKS

    def part(owner, k):
        return pl.ds(pl.multiple_of((owner * CHUNKS + k) * rows, rows), rows)

    mine = col * 2 + core
    across = []
    for k in range(CHUNKS):
        c = copy(m.at[part(mine, k)], pm.at[part(mine, k)], sx.at[k], rx.at[k], (partner, col))
        c.start()
        across.append(c)
    half = pl.ds(pl.multiple_of(core * 512, 512), 512)
    rhs = copy(r.at[half], pr.at[half], sx.at[CHUNKS], rx.at[CHUNKS], (partner, col))
    rhs.start()
    onward, beside = [], []
    for k in range(CHUNKS):
        across[k].wait_recv()
        piece = pm.at[part(mine, k)]
        for d in (1, 3, 2):
            c = copy(piece, piece, sz.at[d - 1, k], rz.at[d - 1, k], (seg, lax.rem(col + d, 4)))
            c.start()
            onward.append((d, k, c))
        c = copy(piece, piece, sd.at[0, k], rd.at[0, k], (sibling, col))
        c.start()
        beside.append(c)
    rhs.wait_recv()
    c = copy(pr.at[half], pr.at[half], sx.at[CHUNKS + 1], rx.at[CHUNKS + 1], (sibling, col))
    c.start()
    beside.append(c)
    for d, k, c in onward:
        c.wait_recv()
        owner = lax.rem(col + 4 - d, 4) * 2 + core
        piece = pm.at[part(owner, k)]
        c = copy(piece, piece, sd.at[d, k], rd.at[d, k], (sibling, col))
        c.start()
        beside.append(c)
    for c in beside:
        c.wait_recv()
    for c in across + [rhs] + [c for _, _, c in onward] + beside:
        c.wait_send()


CHUNKS = 3


def exchange(m, r, level):
    dma = pltpu.SemaphoreType.DMA
    return pl.pallas_call(
        functools.partial(exchange_kernel, level),
        out_shape=shapes(m.shape, r.shape),
        in_specs=[pl.BlockSpec(memory_space=pl.ANY)] * 2,
        out_specs=[pl.BlockSpec(memory_space=pl.ANY)] * 2,
        scratch_shapes=[
            dma((CHUNKS + 2,)), dma((CHUNKS + 2,)), dma((3, CHUNKS)), dma((3, CHUNKS)),
            dma((4, CHUNKS)), dma((4, CHUNKS)),
        ],
        compiler_params=pltpu.CompilerParams(collective_id=level, has_side_effects=True),
    )(m, r)


def all_columns(blocks):
    share = blocks.shape[2]
    around = [blocks]
    for d in (1, 2, 3):
        pairs = [(i, (i - d) % 4) for i in range(4)]
        around.append(lax.ppermute(blocks, "col", pairs))
    twice = jnp.concatenate(around + around[:3], axis=2)
    first = lax.rem(4 - lax.axis_index("col"), 4) * share
    return lax.dynamic_slice_in_dim(twice, first, 4 * share, 2)


def product(a, b):
    return jnp.dot(a, b, precision=lax.Precision.HIGHEST, preferred_element_type=F32)


def on_device(diagonal, lower, right_side):
    size = lower.shape[1]
    seg = lax.axis_index("seg")
    even = all_columns(jnp.stack([diagonal[0], diagonal[2]]))
    odd = all_columns(jnp.stack([diagonal[1], diagonal[3]]))
    left = lower[0] * (seg > 0).astype(F32)
    saved = []
    kept, low = eliminate(even[0], left, lower[1], right_side[0], odd[0], right_side[1])
    saved.append(kept)
    kept, high = eliminate(even[1], lower[2], lower[3], right_side[2], odd[1], right_side[3])
    saved.append(kept)
    kept, state = merge(jnp.zeros((1,), jnp.int32), low, high)
    saved.append(kept)
    for level in range(5):
        ll, lr, rr, rl_, rr_ = state
        m, r = exchange(jnp.concatenate([ll, lr, rr], axis=0), jnp.concatenate([rl_, rr_], axis=0), level)
        other = (m[:size], m[size : 2 * size], m[2 * size :], r[:size], r[size:])
        bit = lax.rem(lax.div(seg, 2**level), 2)
        kept, state = merge(bit.reshape(1).astype(jnp.int32), state, other)
        saved.append(kept)
    right = finish(state[2], state[4])
    lefts = jnp.zeros_like(right)

    def between(kept, a, b):
        g, gf = kept
        return gf - product(g, jnp.concatenate([a, b], axis=0))

    for level in range(4, -1, -1):
        middle = between(saved[3 + level], lefts, right)
        bit = lax.rem(lax.div(seg, 2**level), 2)
        lefts, right = jnp.where(bit == 0, lefts, middle), jnp.where(bit == 0, middle, right)
    second = between(saved[2], lefts, right)
    return jnp.stack([between(saved[0], lefts, second), second, between(saved[1], second, right), right])


def solution(mesh):
    in_specs = (P("seg", None, "col"), P("seg", None, None), P("seg", None, "col"))
    return jax.shard_map(
        on_device, mesh=mesh, in_specs=in_specs, out_specs=P("seg", None, "col"), check_vma=False
    )
```

```python
import functools
import jax
import jax.numpy as jnp
from jax import lax
from jax.experimental import pallas as pl
from jax.experimental.pallas import tpu as pltpu
from jax.sharding import PartitionSpec as P

W = 16
BF = jnp.bfloat16
F32 = jnp.float32


def pieces(x):
    high = x.astype(BF)
    rest = x - high.astype(F32)
    mid = rest.astype(BF)
    low = (rest - mid.astype(F32)).astype(BF)
    return high, mid, low


def beside(h, m, l):
    return jnp.concatenate([h, m, h, m, h, l], axis=1)


def below(h, m, l):
    return jnp.concatenate([h, h, m, m, l, h], axis=0)


def dot(a, b):
    return jnp.dot(a, b, preferred_element_type=F32)


def at(i, size):
    return pl.ds(pl.multiple_of(i * size, size), size)


def invert128(block):
    sub = lax.broadcasted_iota(jnp.int32, (W, 128), 0)
    lane = lax.broadcasted_iota(jnp.int32, (W, 128), 1)
    count = 128 // W
    panels = [block[W * i : W * i + W] for i in range(count)]
    for k in range(count):
        first = W * k
        rows = panels[k]
        cols = [jnp.broadcast_to(rows[:, first + p : first + p + 1], (W, 128)) for p in range(W)]
        inside = (lane >= first) & (lane < first + W)
        after = k + 1 if k + 1 < count else None
        if after is not None:
            wide = [
                jnp.broadcast_to(panels[after][:, first + p : first + p + 1], (W, 128)) for p in range(W)
            ]
        rest = [i for i in range(count) if i not in (k, after)]
        left = beside(*pieces(jnp.concatenate([panels[i] for i in rest], axis=0)))
        rows = jnp.where(inside, (lane - first == sub).astype(F32), rows)
        diag = cols[0][0:1, :]
        for p in range(W):
            pivot = 1.0 / diag
            here = sub == p
            column = cols[p]
            for j in range(p + 1, W):
                if j == p + 1:
                    moved = cols[j] - (column * cols[j][p : p + 1, :]) * pivot
                    diag = moved[j : j + 1, :]
                    cols[j] = jnp.where(here, cols[j][p : p + 1, :] * pivot, moved)
                else:
                    scaled = cols[j][p : p + 1, :] * pivot
                    cols[j] = jnp.where(here, scaled, cols[j] - column * scaled)
            scaled = rows[p : p + 1, :] * pivot
            rows = jnp.where(here, scaled, rows - column * scaled)
        if after is not None:
            acc = jnp.where(inside, 0.0, panels[after])
            for p in range(W):
                acc = acc - wide[p] * rows[p : p + 1, :]
        padded = [
            jnp.concatenate(
                [jnp.zeros((first, 128), BF)] * (first > 0)
                + [q]
                + [jnp.zeros((112 - first, 128), BF)] * (first < 112),
                axis=0,
            )
            for q in pieces(rows)
        ]
        delta = dot(left, below(*padded))
        for n, i in enumerate(rest):
            panels[i] = jnp.where(inside, 0.0, panels[i]) - delta[W * n : W * n + W]
        panels[k] = rows
        if after is not None:
            panels[after] = acc
    return jnp.concatenate(panels, axis=0)


MESH_ID = pl.DeviceIdType.MESH


def partner_of(seg, level):
    if level == 0:
        return seg + 1 - 2 * lax.rem(seg, 2)
    core, x, y = lax.rem(seg, 2), lax.rem(lax.div(seg, 2), 4), lax.div(seg, 8)
    if level == 1:
        x = x + 1 - 2 * lax.rem(x, 2)
    if level == 2:
        x = 3 - x
    if level == 3:
        y = y + 1 - 2 * lax.rem(y, 2)
    if level == 4:
        y = 3 - y
    return (y * 4 + x) * 2 + core


def invert(p, hook):
    def step(j, c):
        hook(j)
        s = at(j, 128)
        w = invert128(p[s, s])
        rowid = lax.broadcasted_iota(jnp.int32, (512, 1), 0) // 128
        u6 = beside(*pieces(jnp.where(rowid == j, 0.0, p[:, s])))
        w6 = beside(*pieces(w))
        t = dot(w6, below(*pieces(p[s, :])))
        here = lax.broadcasted_iota(jnp.int32, (1, 512), 1) // 128 == j
        t = jnp.where(here, jnp.concatenate([w] * 4, axis=1), t)
        for n in (slice(0, 256), slice(256, 512)):
            p[:, n] = jnp.where(here[:, n], 0.0, p[:, n]) - dot(u6, below(*pieces(t[:, n])))
        p[s, :] = t
        return c

    lax.fori_loop(0, 4, step, 0)


def kernel(
    diag, low, right, x,
    dv, lv, rv, st, rh, p, p3, e, f, et, gg, gl, gf, fp, xs, keep,
    load_sem, ds, dr, xsend, xrecv, zsend, zrecv, csend, crecv, ready,
):
    seg, col = lax.axis_index("seg"), lax.axis_index("col")
    core = lax.rem(seg, 2)
    me = col * 2 + core
    sibling = (partner_of(seg, 0), col)
    around = [(seg, lax.rem(col + d, 4)) for d in (1, 2, 3)]
    across = [(partner_of(seg, level), col) for level in range(1, 5)]

    def remote(src, dst, s, d, peer):
        return pltpu.make_async_remote_copy(
            src_ref=src, dst_ref=dst, send_sem=s, recv_sem=d, device_id=peer, device_id_type=MESH_ID
        )

    columns = pl.ds(pl.multiple_of(col * 128, 128), 128)
    loads = [pltpu.make_async_copy(low.at[b], lv.at[b], load_sem.at[b]) for b in range(4)]
    loads.append(pltpu.make_async_copy(right, rv, load_sem.at[4]))
    own = [pltpu.make_async_copy(diag.at[b], dv.at[b, :, columns], load_sem.at[5 + b]) for b in range(4)]
    for c in [own[0], loads[0], loads[1], loads[4], own[2], loads[2], loads[3], own[1], own[3]]:
        c.start()
    barrier = pltpu.get_barrier_semaphore()
    for peer in [sibling] + around + across:
        pl.semaphore_signal(barrier, inc=1, device_id=peer, device_id_type=MESH_ID)
    pl.semaphore_wait(barrier, 8)
    slabs = [
        [
            remote(diag.at[b], dv.at[b, :, columns], ds.at[b, d], dr.at[b, d], around[d])
            for d in (0, 2, 1)
        ]
        for b in range(4)
    ]
    for b in (0, 2, 1, 3):
        for c in slabs[b]:
            c.start()

    def arrived(b):
        own[b].wait()
        for c in slabs[b]:
            c.wait_recv()

    def node(n, power):
        other = 1 + lax.rem(n + 1, 2)
        bit = lax.rem(lax.div(seg, power), 2) * (n >= 3).astype(jnp.int32)
        a, b = bit * other, (1 - bit) * other
        par = lax.rem(n + 1, 2)

        def rows(base, i, size):
            return pl.ds(pl.multiple_of(base + i * size, size), size)

        def crossing(to, there):
            s, d = bit * 1024, (1 - bit) * 1024
            if there:
                s, d = d, s
            half = 512 * bit
            if there:
                half = 512 - half
            src, dst = (0, other) if there else (other, other)
            list_ = [
                (st.at[src, rows(s, core, 128)], st.at[dst, rows(s, core, 128)]),
                (st.at[src, rows(s + 256, core, 128), 256:512], st.at[dst, rows(s + 256, core, 128), 256:512]),
                (st.at[src, rows(512, me, 64)], st.at[dst, rows(512, me, 64)]),
                (rh.at[src, rows(half, core, 256)], rh.at[dst, rows(half, core, 256)]),
                (st.at[src, rows(d, me, 64)], st.at[dst, rows(d, me, 64)]),
                (rh.at[src, rows(512 - half, core, 256)], rh.at[dst, rows(512 - half, core, 256)]),
            ]
            return [remote(u, v, xsend.at[par, i], xrecv.at[par, i], to) for i, (u, v) in enumerate(list_)]

        def whole(there):
            s, d, half = bit * 1024, (1 - bit) * 1024, 512 * bit
            if there:
                s, d, half = d, s, 512 - half
            src = 0 if there else other
            list_ = [
                (st.at[src, rows(s, 0, 512)], st.at[other, rows(s, 0, 512)]),
                (st.at[src, rows(512, 0, 512)], st.at[other, rows(512, 0, 512)]),
                (rh.at[src, rows(half, 0, 512)], rh.at[other, rows(half, 0, 512)]),
                (st.at[src, rows(d, 0, 512)], st.at[other, rows(d, 0, 512)]),
                (rh.at[src, rows(512 - half, 0, 512)], rh.at[other, rows(512 - half, 0, 512)]),
            ]
            return [remote(u, v, xsend.at[par, i], xrecv.at[par, i], sibling) for i, (u, v) in enumerate(list_)]

        came = crossing(sibling, False)

        s_, d_, half_ = bit * 1024, (1 - bit) * 1024, 512 * bit
        got = [
            st.at[other, rows(s_, core, 128)],
            st.at[other, rows(s_ + 256, core, 128), 256:512],
            st.at[other, rows(512, me, 64)],
            rh.at[other, rows(half_, core, 256)],
            st.at[other, rows(d_, me, 64)],
            rh.at[other, rows(512 - half_, core, 256)],
        ]

        def to_sibling(i, ref):
            return remote(ref, ref, csend.at[par, i], crecv.at[par, i], sibling)

        def round_z(kind):
            i = 2 + 2 * kind
            return [
                remote(got[i], got[i], zsend.at[par, kind, d], zrecv.at[par, kind, d], around[d])
                for d in range(3)
            ]

        def from_z(kind):
            base = 512 if kind == 0 else d_
            out = []
            for d in range(3):
                owner = lax.rem(col + 3 - d, 4) * 2 + core
                ref = st.at[other, rows(base, owner, 64)]
                out.append(to_sibling(6 + 3 * kind + d, ref))
            return out

        direct = [to_sibling(i, got[i]) for i in range(6)]
        far = n >= 4

        def hook(j):
            @pl.when(far & (j == 1))
            def _():
                came[2].wait_recv()
                for c in round_z(0):
                    c.start()
                direct[2].start()

            @pl.when(far & (j == 2))
            def _():
                came[3].wait_recv()
                direct[3].start()

            @pl.when(far & (j == 3))
            def _():
                came[4].wait_recv()
                for c in round_z(1):
                    c.start()
                direct[4].start()
                for c, onward in zip(round_z(0), from_z(0)):
                    c.wait_recv()
                    onward.start()

        @pl.when(n == 0)
        def _():
            arrived(0)
            p[...] = dv[0]

        @pl.when(n == 1)
        def _():
            arrived(2)
            p[...] = dv[2]

        @pl.when(n == 2)
        def _():
            arrived(1)
            arrived(3)

        @pl.when(n == 3)
        def _():
            for c in whole(True):
                c.start()
            whole(False)[0].wait_recv()

        for level in range(1, 5):

            @pl.when(n == 3 + level)
            def _(level=level):
                pl.semaphore_wait(ready.at[level], 5)
                for c in crossing(across[level - 1], True):
                    c.start()

        @pl.when(far & (n < 8))
        def _():
            for i in (0, 1):
                came[i].wait_recv()
                direct[i].start()
            for i in (0, 1):
                direct[i].wait_recv()

        @pl.when((n >= 2) & (n < 8))
        def _():
            p[...] = st[a, 1024:1536, :] + st[b, 0:512, :]

        @pl.when(n == 2)
        def _():
            p[...] = p[...] + dv[1]

        @pl.when(n == 8)
        def _():
            p[...] = st[0, 1024:1536, :]

        p[256:512, 0:256] = p[0:256, 256:512].T
        invert(p, lambda j: pl.when(n < 8)(lambda: hook(j)))

        @pl.when(n < 8)
        def _():
            @pl.when(n == 0)
            def _():
                loads[0].wait()
                loads[1].wait()
                loads[4].wait()

            @pl.when(n == 1)
            def _():
                loads[2].wait()
                loads[3].wait()

            @pl.when(n < 2)
            def _():
                q = 2 * n
                has_left = 1.0 - ((n == 0) & (seg == 0)).astype(F32)
                et[512:1024, :] = lv[q + 1]
                e[:, 0:512] = lv[q] * has_left
                et[0:512, :] = e[:, 0:512].T
                e[:, 512:1024] = et[512:1024, :].T
                f[...] = rv[q]
                st[q] = jnp.zeros((1536, 512), F32)
                rh[q] = jnp.zeros((1024, 128), F32)

            @pl.when(n == 3)
            def _():
                for c in whole(False)[1:3]:
                    c.wait_recv()

            @pl.when(far)
            def _():
                for c in direct[2:4] + from_z(0):
                    c.wait_recv()

            @pl.when(n >= 2)
            def _():
                et[0:512, :] = st[a, 512:1024, :]
                e[:, 512:1024] = st[b, 512:1024, :]
                e[:, 0:512] = et[0:512, :].T
                et[512:1024, :] = e[:, 512:1024].T
                f[...] = rh[a, 512:1024, :] + rh[b, 0:512, :]

            @pl.when(n == 2)
            def _():
                f[...] = f[...] + rv[1]

            for q, part in enumerate(pieces(p[...])):
                p3[q] = part

            def tile(i, c):
                k = at(i, 256)
                out = dot(beside(p3[0], p3[1], p3[2]), below(*pieces(e[:, k])))
                gg[n, 0, :, k], gg[n, 1, :, k], gl[:, k] = pieces(out)
                return c

            lax.fori_loop(0, 4, tile, 0)
            fh, fm, _ = pieces(f[...])
            out = dot(
                jnp.concatenate([p3[0], p3[1], p3[0]], axis=1), jnp.concatenate([fh, fh, fm], axis=0)
            )
            gf[n] = out
            fp[0], fp[1], _ = pieces(out)

            @pl.when(n == 3)
            def _():
                for c in whole(False)[3:]:
                    c.wait_recv()
                for c in whole(True):
                    c.wait_send()

            @pl.when(far)
            def _():
                came[5].wait_recv()
                direct[5].start()
                for c, onward in zip(round_z(1), from_z(1)):
                    c.wait_recv()
                    onward.start()
                for c in direct[4:6] + from_z(1):
                    c.wait_recv()
                for c in crossing(sibling, True) + direct + round_z(0) + round_z(1) + from_z(0) + from_z(1):
                    c.wait_send()

            @pl.when(n >= 2)
            def _():
                r = pl.ds(pl.multiple_of((1 - bit) * 1024, 512), 512)
                st[0, r, :] = st[other, r, :]
                r = pl.ds(pl.multiple_of((1 - bit) * 512, 512), 512)
                rh[0, r, :] = rh[other, r, :]

            @pl.when(n == 2)
            def _():
                st[0, 1024:1536, :] = st[0, 1024:1536, :] + dv[3]
                rh[0, 512:1024, :] = rh[0, 512:1024, :] + rv[3]

            t = 2 * (n == 1).astype(jnp.int32)

            def term(i, k):
                k = at(k, 256)
                return dot(beside(*pieces(et[at(i, 256), :])), below(gg[n, 0, :, k], gg[n, 1, :, k], gl[:, k]))

            def corner(q, c):
                i, k = q // 2, at((q + 1) // 2, 256)
                st[t, at(i + 4, 256), k] = st[t, at(i + 4, 256), k] - term(i + 2, (q + 1) // 2 + 2)
                return c

            lax.fori_loop(0, 3, corner, 0)
            st[t, 1280:1536, 0:256] = st[t, 1024:1280, 256:512].T

            @pl.when(n < 7)
            def _():
                def corner(q, c):
                    i, k = q // 2, at((q + 1) // 2, 256)
                    st[t, at(i, 256), k] = st[t, at(i, 256), k] - term(i, (q + 1) // 2)
                    return c

                lax.fori_loop(0, 3, corner, 0)
                st[t, 256:512, 0:256] = st[t, 0:256, 256:512].T

                def square(q, c):
                    i, k = q // 2, q % 2
                    st[t, at(i + 2, 256), at(k, 256)] = -term(i, k + 2)
                    return c

                lax.fori_loop(0, 4, square, 0)

            def side(i, c):
                r = at(i, 256)
                h, m, _ = pieces(et[r, :])
                rh[t, r, :] = rh[t, r, :] - dot(
                    jnp.concatenate([h, m, h], axis=1), jnp.concatenate([fp[0], fp[0], fp[1]], axis=0)
                )
                return c

            lax.fori_loop(0, 4, side, 0)
            for level in range(1, 5):

                @pl.when(n == level + 1)
                def _(level=level):
                    for peer in [sibling, across[level - 1]] + around:
                        pl.semaphore_signal(
                            ready.at[level], inc=1, device_id=peer, device_id_type=MESH_ID
                        )

        return power * (1 + (n >= 3).astype(jnp.int32))

    lax.fori_loop(0, 9, node, jnp.int32(1))
    for b in range(4):
        for c in slabs[b]:
            c.wait_send()
    xs[0:512, :] = jnp.zeros((512, 128), F32)
    last = dot(beside(*pieces(p[...])), below(*pieces(rh[0, 512:1024, :])))
    xs[512:1024, :] = last
    x[3] = jnp.zeros((512, 128), F32)

    def back(i, power):
        n = 7 - i
        h, m, _ = pieces(xs[...])
        middle = gf[n] - dot(
            jnp.concatenate([gg[n, 0], gg[n, 1], gg[n, 0]], axis=1), jnp.concatenate([h, h, m], axis=0)
        )

        @pl.when(n >= 3)
        def _():
            bit = lax.rem(lax.div(seg, power), 2)
            xs[pl.ds(pl.multiple_of((1 - bit) * 512, 512), 512), :] = middle

        @pl.when(n == 2)
        def _():
            x[3] = xs[512:1024, :]
            x[1] = middle
            keep[...] = xs[0:512, :]
            xs[0:512, :] = middle

        @pl.when(n == 1)
        def _():
            x[2] = middle
            xs[512:1024, :] = xs[0:512, :]
            xs[0:512, :] = keep[...]

        @pl.when(n == 0)
        def _():
            x[0] = middle

        return power // (1 + (n > 3).astype(jnp.int32))

    lax.fori_loop(0, 8, back, jnp.int32(16))


def on_device(diagonal, lower, right_side):
    dma = pltpu.SemaphoreType.DMA
    vmem = pltpu.VMEM
    return pl.pallas_call(
        kernel,
        out_shape=jax.ShapeDtypeStruct((4, 512, 128), F32),
        in_specs=[pl.BlockSpec(memory_space=pl.ANY)] * 3,
        out_specs=pl.BlockSpec(memory_space=pltpu.VMEM),
        scratch_shapes=[
            vmem((4, 512, 512), F32), vmem((4, 512, 512), F32), vmem((4, 512, 128), F32),
            vmem((3, 1536, 512), F32), vmem((3, 1024, 128), F32),
            vmem((512, 512), F32), vmem((3, 512, 512), BF), vmem((512, 1024), F32),
            vmem((512, 128), F32), vmem((1024, 512), F32),
            vmem((8, 2, 512, 1024), BF), vmem((512, 1024), BF), vmem((8, 512, 128), F32),
            vmem((2, 512, 128), BF), vmem((1024, 128), F32), vmem((512, 128), F32),
            dma((9,)), dma((4, 3)), dma((4, 3)),
            dma((2, 6)), dma((2, 6)), dma((2, 2, 3)), dma((2, 2, 3)), dma((2, 12)), dma((2, 12)),
            pltpu.SemaphoreType.REGULAR((5,)),
        ],
        compiler_params=pltpu.CompilerParams(
            collective_id=0, has_side_effects=True, vmem_limit_bytes=64000 * 1024
        ),
    )(diagonal, lower, right_side)


def solution(mesh):
    in_specs = (P("seg", None, "col"), P("seg", None, None), P("seg", None, "col"))
    return jax.shard_map(
        on_device, mesh=mesh, in_specs=in_specs, out_specs=P("seg", None, "col"), check_vma=False
    )
```

```python
import functools
import jax
import jax.numpy as jnp
from jax import lax
from jax.experimental import pallas as pl
from jax.experimental.pallas import tpu as pltpu
from jax.sharding import PartitionSpec as P

W = 16
BF = jnp.bfloat16
F32 = jnp.float32


def pieces(x):
    high = x.astype(BF)
    rest = x - high.astype(F32)
    mid = rest.astype(BF)
    low = (rest - mid.astype(F32)).astype(BF)
    return high, mid, low


def beside(h, m, l):
    return jnp.concatenate([h, m, h, m, h, l], axis=1)


def below(h, m, l):
    return jnp.concatenate([h, h, m, m, l, h], axis=0)


def dot(a, b):
    return jnp.dot(a, b, preferred_element_type=F32)


def at(i, size):
    return pl.ds(pl.multiple_of(i * size, size), size)


def invert128(block):
    sub = lax.broadcasted_iota(jnp.int32, (W, 128), 0)
    lane = lax.broadcasted_iota(jnp.int32, (W, 128), 1)
    count = 128 // W
    panels = [block[W * i : W * i + W] for i in range(count)]
    for k in range(count):
        first = W * k
        rows = panels[k]
        cols = [jnp.broadcast_to(rows[:, first + p : first + p + 1], (W, 128)) for p in range(W)]
        inside = (lane >= first) & (lane < first + W)
        after = k + 1 if k + 1 < count else None
        if after is not None:
            wide = [
                jnp.broadcast_to(panels[after][:, first + p : first + p + 1], (W, 128)) for p in range(W)
            ]
        rest = [i for i in range(count) if i not in (k, after)]
        left = beside(*pieces(jnp.concatenate([panels[i] for i in rest], axis=0)))
        rows = jnp.where(inside, (lane - first == sub).astype(F32), rows)
        diag = cols[0][0:1, :]
        for p in range(W):
            pivot = 1.0 / diag
            here = sub == p
            column = cols[p]
            for j in range(p + 1, W):
                if j == p + 1:
                    moved = cols[j] - (column * cols[j][p : p + 1, :]) * pivot
                    diag = moved[j : j + 1, :]
                    cols[j] = jnp.where(here, cols[j][p : p + 1, :] * pivot, moved)
                else:
                    scaled = cols[j][p : p + 1, :] * pivot
                    cols[j] = jnp.where(here, scaled, cols[j] - column * scaled)
            scaled = rows[p : p + 1, :] * pivot
            rows = jnp.where(here, scaled, rows - column * scaled)
        if after is not None:
            acc = jnp.where(inside, 0.0, panels[after])
            for p in range(W):
                acc = acc - wide[p] * rows[p : p + 1, :]
        padded = [
            jnp.concatenate(
                [jnp.zeros((first, 128), BF)] * (first > 0)
                + [q]
                + [jnp.zeros((112 - first, 128), BF)] * (first < 112),
                axis=0,
            )
            for q in pieces(rows)
        ]
        delta = dot(left, below(*padded))
        for n, i in enumerate(rest):
            panels[i] = jnp.where(inside, 0.0, panels[i]) - delta[W * n : W * n + W]
        panels[k] = rows
        if after is not None:
            panels[after] = acc
    return jnp.concatenate(panels, axis=0)


MESH_ID = pl.DeviceIdType.MESH


def partner_of(seg, level):
    if level == 0:
        return seg + 1 - 2 * lax.rem(seg, 2)
    core, x, y = lax.rem(seg, 2), lax.rem(lax.div(seg, 2), 4), lax.div(seg, 8)
    if level == 1:
        x = x + 1 - 2 * lax.rem(x, 2)
    if level == 2:
        x = 3 - x
    if level == 3:
        y = y + 1 - 2 * lax.rem(y, 2)
    if level == 4:
        y = 3 - y
    return (y * 4 + x) * 2 + core


def invert(p, hook):
    def step(j, c):
        hook(j)
        s = at(j, 128)
        w = invert128(p[s, s])
        rowid = lax.broadcasted_iota(jnp.int32, (512, 1), 0) // 128
        u6 = beside(*pieces(jnp.where(rowid == j, 0.0, p[:, s])))
        w6 = beside(*pieces(w))
        t = dot(w6, below(*pieces(p[s, :])))
        here = lax.broadcasted_iota(jnp.int32, (1, 512), 1) // 128 == j
        t = jnp.where(here, jnp.concatenate([w] * 4, axis=1), t)
        for n in (slice(0, 256), slice(256, 512)):
            p[:, n] = jnp.where(here[:, n], 0.0, p[:, n]) - dot(u6, below(*pieces(t[:, n])))
        p[s, :] = t
        return c

    lax.fori_loop(0, 4, step, 0)


def kernel(
    diag, low, right, x,
    dv, lv, rv, st, rh, p, p3, e, f, et, gg, gl, gf, fp, xs, keep,
    load_sem, ds, dr, xsend, xrecv, zsend, zrecv, csend, crecv, ready,
):
    seg, col = lax.axis_index("seg"), lax.axis_index("col")
    core = lax.rem(seg, 2)
    me = col * 2 + core
    sibling = (partner_of(seg, 0), col)
    around = [(seg, lax.rem(col + d, 4)) for d in (1, 2, 3)]
    across = [(partner_of(seg, level), col) for level in range(1, 5)]

    def remote(src, dst, s, d, peer):
        return pltpu.make_async_remote_copy(
            src_ref=src, dst_ref=dst, send_sem=s, recv_sem=d, device_id=peer, device_id_type=MESH_ID
        )

    columns = pl.ds(pl.multiple_of(col * 128, 128), 128)
    loads = [pltpu.make_async_copy(low.at[b], lv.at[b], load_sem.at[b]) for b in range(4)]
    loads.append(pltpu.make_async_copy(right, rv, load_sem.at[4]))
    own = [pltpu.make_async_copy(diag.at[b], dv.at[b, :, columns], load_sem.at[5 + b]) for b in range(4)]
    for c in [own[0], loads[0], loads[1], loads[4], own[2], loads[2], loads[3], own[1], own[3]]:
        c.start()
    barrier = pltpu.get_barrier_semaphore()
    for peer in [sibling] + around + across:
        pl.semaphore_signal(barrier, inc=1, device_id=peer, device_id_type=MESH_ID)
    pl.semaphore_wait(barrier, 8)
    upper = lax.div(col, 2)
    third = (1 - upper) * (3 - col) + upper * (col - 2)
    shares = [
        pl.ds(pl.multiple_of(upper * 256, 256), 256),
        pl.ds(pl.multiple_of(third * 128, 128), 128),
    ]
    slabs = [
        [
            remote(diag.at[b, r], dv.at[b, r, columns], ds.at[b, d, i], dr.at[b, d, i], around[d])
            for d in (0, 2, 1)
            for i, r in enumerate(shares)
        ]
        for b in range(4)
    ]
    for b in (0, 2, 1, 3):
        for c in slabs[b]:
            c.start()

    def arrived(b):
        own[b].wait()
        for c in slabs[b]:
            c.wait_recv()
        dv[b, 0:128, 384:512] = dv[b, 384:512, 0:128].T
        dv[b, 128:256, 256:384] = dv[b, 256:384, 128:256].T

    def node(n, power):
        other = 1 + lax.rem(n + 1, 2)
        bit = lax.rem(lax.div(seg, power), 2) * (n >= 3).astype(jnp.int32)
        a, b = bit * other, (1 - bit) * other
        par = lax.rem(n + 1, 2)

        def rows(base, i, size):
            return pl.ds(pl.multiple_of(base + i * size, size), size)

        def crossing(to, there, bit=bit, other=other, par=par):
            s, d = bit * 1024, (1 - bit) * 1024
            if there:
                s, d = d, s
            half = 512 * bit
            if there:
                half = 512 - half
            src, dst = (0, other) if there else (other, other)
            list_ = [
                (st.at[src, rows(s, core, 128)], st.at[dst, rows(s, core, 128)]),
                (st.at[src, rows(s + 256, core, 128), 256:512], st.at[dst, rows(s + 256, core, 128), 256:512]),
                (st.at[src, rows(512, me, 64)], st.at[dst, rows(512, me, 64)]),
                (rh.at[src, rows(half, core, 256)], rh.at[dst, rows(half, core, 256)]),
                (st.at[src, rows(d, me, 64)], st.at[dst, rows(d, me, 64)]),
                (rh.at[src, rows(512 - half, core, 256)], rh.at[dst, rows(512 - half, core, 256)]),
            ]
            return [remote(u, v, xsend.at[par, i], xrecv.at[par, i], to) for i, (u, v) in enumerate(list_)]

        def whole(there, bit=bit, other=other, par=par):
            s, d, half = bit * 1024, (1 - bit) * 1024, 512 * bit
            if there:
                s, d, half = d, s, 512 - half
            src = 0 if there else other
            list_ = [
                (st.at[src, rows(s, 0, 512)], st.at[other, rows(s, 0, 512)]),
                (st.at[src, rows(512, 0, 512)], st.at[other, rows(512, 0, 512)]),
                (rh.at[src, rows(half, 0, 512)], rh.at[other, rows(half, 0, 512)]),
                (st.at[src, rows(d, 0, 512)], st.at[other, rows(d, 0, 512)]),
                (rh.at[src, rows(512 - half, 0, 512)], rh.at[other, rows(512 - half, 0, 512)]),
            ]
            return [remote(u, v, xsend.at[par, i], xrecv.at[par, i], sibling) for i, (u, v) in enumerate(list_)]

        came = crossing(sibling, False)

        s_, d_, half_ = bit * 1024, (1 - bit) * 1024, 512 * bit
        got = [
            st.at[other, rows(s_, core, 128)],
            st.at[other, rows(s_ + 256, core, 128), 256:512],
            st.at[other, rows(512, me, 64)],
            rh.at[other, rows(half_, core, 256)],
            st.at[other, rows(d_, me, 64)],
            rh.at[other, rows(512 - half_, core, 256)],
        ]

        def to_sibling(i, ref):
            return remote(ref, ref, csend.at[par, i], crecv.at[par, i], sibling)

        def round_z(kind):
            i = 2 + 2 * kind
            return [
                remote(got[i], got[i], zsend.at[par, kind, d], zrecv.at[par, kind, d], around[d])
                for d in range(3)
            ]

        def from_z(kind):
            base = 512 if kind == 0 else d_
            out = []
            for d in range(3):
                owner = lax.rem(col + 3 - d, 4) * 2 + core
                ref = st.at[other, rows(base, owner, 64)]
                out.append(to_sibling(6 + 3 * kind + d, ref))
            return out

        direct = [to_sibling(i, got[i]) for i in range(6)]
        far = n >= 4

        def hook(j):
            @pl.when(far & (j == 1))
            def _():
                came[2].wait_recv()
                for c in round_z(0):
                    c.start()
                direct[2].start()

            @pl.when(far & (j == 2))
            def _():
                came[3].wait_recv()
                direct[3].start()

            @pl.when(far & (j == 3))
            def _():
                came[4].wait_recv()
                for c in round_z(1):
                    c.start()
                direct[4].start()
                for c, onward in zip(round_z(0), from_z(0)):
                    c.wait_recv()
                    onward.start()

        @pl.when(n == 0)
        def _():
            loads[0].wait()
            loads[1].wait()
            loads[4].wait()

        @pl.when(n == 1)
        def _():
            loads[2].wait()
            loads[3].wait()

        @pl.when(n < 2)
        def _():
            q = 2 * n
            has_left = 1.0 - ((n == 0) & (seg == 0)).astype(F32)
            et[512:1024, :] = lv[q + 1]
            e[:, 0:512] = lv[q] * has_left
            et[0:512, :] = e[:, 0:512].T
            e[:, 512:1024] = et[512:1024, :].T
            f[...] = rv[q]
            st[q] = jnp.zeros((1536, 512), F32)
            rh[q] = jnp.zeros((1024, 128), F32)

        @pl.when(n == 0)
        def _():
            arrived(0)
            p[...] = dv[0]

        @pl.when(n == 1)
        def _():
            arrived(2)
            p[...] = dv[2]

        @pl.when(n == 2)
        def _():
            arrived(1)
            arrived(3)

        @pl.when(n == 3)
        def _():
            whole(False)[0].wait_recv()

        @pl.when(far & (n < 8))
        def _():
            for i in (0, 1):
                came[i].wait_recv()
                direct[i].start()
            for i in (0, 1):
                direct[i].wait_recv()

        @pl.when((n >= 2) & (n < 8))
        def _():
            p[...] = st[a, 1024:1536, :] + st[b, 0:512, :]

        @pl.when(n == 2)
        def _():
            p[...] = p[...] + dv[1]

        @pl.when(n == 8)
        def _():
            p[...] = st[0, 1024:1536, :]

        p[256:512, 0:256] = p[0:256, 256:512].T
        invert(p, lambda j: pl.when(n < 8)(lambda: hook(j)))

        @pl.when(n < 8)
        def _():
            @pl.when(n == 3)
            def _():
                for c in whole(False)[1:3]:
                    c.wait_recv()

            @pl.when(far)
            def _():
                for c in direct[2:4] + from_z(0):
                    c.wait_recv()

            @pl.when(n >= 2)
            def _():
                et[0:512, :] = st[a, 512:1024, :]
                e[:, 512:1024] = st[b, 512:1024, :]
                e[:, 0:512] = et[0:512, :].T
                et[512:1024, :] = e[:, 512:1024].T
                f[...] = rh[a, 512:1024, :] + rh[b, 0:512, :]

            @pl.when(n == 2)
            def _():
                f[...] = f[...] + rv[1]

            for q, part in enumerate(pieces(p[...])):
                p3[q] = part

            def tile(i, c):
                k = at(i, 256)
                out = dot(beside(p3[0], p3[1], p3[2]), below(*pieces(e[:, k])))
                gg[n, 0, :, k], gg[n, 1, :, k], gl[:, k] = pieces(out)
                return c

            lax.fori_loop(0, 4, tile, 0)
            fh, fm, _ = pieces(f[...])
            out = dot(
                jnp.concatenate([p3[0], p3[1], p3[0]], axis=1), jnp.concatenate([fh, fh, fm], axis=0)
            )
            gf[n] = out
            fp[0], fp[1], _ = pieces(out)

            @pl.when(n == 3)
            def _():
                for c in whole(False)[3:]:
                    c.wait_recv()
                for c in whole(True):
                    c.wait_send()

            @pl.when(far)
            def _():
                came[5].wait_recv()
                direct[5].start()
                for c, onward in zip(round_z(1), from_z(1)):
                    c.wait_recv()
                    onward.start()
                for c in direct[4:6] + from_z(1):
                    c.wait_recv()
                for c in crossing(sibling, True) + direct + round_z(0) + round_z(1) + from_z(0) + from_z(1):
                    c.wait_send()

            @pl.when(n >= 2)
            def _():
                r = pl.ds(pl.multiple_of((1 - bit) * 1024, 512), 512)
                st[0, r, :] = st[other, r, :]
                r = pl.ds(pl.multiple_of((1 - bit) * 512, 512), 512)
                rh[0, r, :] = rh[other, r, :]

            @pl.when(n == 2)
            def _():
                st[0, 1024:1536, :] = st[0, 1024:1536, :] + dv[3]
                rh[0, 512:1024, :] = rh[0, 512:1024, :] + rv[3]

            t = 2 * (n == 1).astype(jnp.int32)

            def term(i, k):
                k = at(k, 256)
                return dot(beside(*pieces(et[at(i, 256), :])), below(gg[n, 0, :, k], gg[n, 1, :, k], gl[:, k]))

            following = power * (1 + (n >= 3).astype(jnp.int32))
            sends = (n >= 2) & (n < 7)
            turn = lax.rem(lax.div(seg, following), 2)
            first = 1 - turn * sends.astype(jnp.int32)
            to = dict(bit=turn, other=1 + lax.rem(n, 2), par=lax.rem(n, 2))

            def send(part):
                @pl.when(n == 2)
                def _():
                    for c in whole(True, **to)[:1] if part == 0 else whole(True, **to)[1:]:
                        c.start()

                for level in range(1, 5):

                    @pl.when(n == 2 + level)
                    def _(level=level):
                        out = crossing(across[level - 1], True, **to)
                        if part == 0:
                            pl.semaphore_wait(ready.at[level], 5)
                        for c in out[:2] if part == 0 else out[2:]:
                            c.start()

            def corners(turned, c):
                w = first + turned * (1 - 2 * first)

                def corner(q, c):
                    i, k = q // 2 + 4 * w, (q + 1) // 2
                    r = at(i, 256)
                    st[t, r, at(k, 256)] = st[t, r, at(k, 256)] - term(q // 2 + 2 * w, k + 2 * w)
                    return c

                lax.fori_loop(0, 3, corner, 0)
                st[t, at(4 * w + 1, 256), 0:256] = st[t, at(4 * w, 256), 256:512].T
                pl.when(turned == 0)(lambda: send(0))
                return c

            lax.fori_loop(0, 2 - (n == 7).astype(jnp.int32), corners, 0)

            @pl.when(n < 7)
            def _():
                def square(q, c):
                    i, k = q // 2, q % 2
                    st[t, at(i + 2, 256), at(k, 256)] = -term(i, k + 2)
                    return c

                lax.fori_loop(0, 4, square, 0)

            def side(i, c):
                r = at(i, 256)
                h, m, _ = pieces(et[r, :])
                rh[t, r, :] = rh[t, r, :] - dot(
                    jnp.concatenate([h, m, h], axis=1), jnp.concatenate([fp[0], fp[0], fp[1]], axis=0)
                )
                return c

            lax.fori_loop(0, 4, side, 0)
            send(1)
            for level in range(1, 5):

                @pl.when(n == level + 1)
                def _(level=level):
                    for peer in [sibling, across[level - 1]] + around:
                        pl.semaphore_signal(
                            ready.at[level], inc=1, device_id=peer, device_id_type=MESH_ID
                        )

        return power * (1 + (n >= 3).astype(jnp.int32))

    lax.fori_loop(0, 9, node, jnp.int32(1))
    for b in range(4):
        for c in slabs[b]:
            c.wait_send()
    xs[0:512, :] = jnp.zeros((512, 128), F32)
    last = dot(beside(*pieces(p[...])), below(*pieces(rh[0, 512:1024, :])))
    xs[512:1024, :] = last
    x[3] = jnp.zeros((512, 128), F32)

    def back(i, power):
        n = 7 - i
        h, m, _ = pieces(xs[...])
        middle = gf[n] - dot(
            jnp.concatenate([gg[n, 0], gg[n, 1], gg[n, 0]], axis=1), jnp.concatenate([h, h, m], axis=0)
        )

        @pl.when(n >= 3)
        def _():
            bit = lax.rem(lax.div(seg, power), 2)
            xs[pl.ds(pl.multiple_of((1 - bit) * 512, 512), 512), :] = middle

        @pl.when(n == 2)
        def _():
            x[3] = xs[512:1024, :]
            x[1] = middle
            keep[...] = xs[0:512, :]
            xs[0:512, :] = middle

        @pl.when(n == 1)
        def _():
            x[2] = middle
            xs[512:1024, :] = xs[0:512, :]
            xs[0:512, :] = keep[...]

        @pl.when(n == 0)
        def _():
            x[0] = middle

        return power // (1 + (n > 3).astype(jnp.int32))

    lax.fori_loop(0, 8, back, jnp.int32(16))


def on_device(diagonal, lower, right_side):
    dma = pltpu.SemaphoreType.DMA
    vmem = pltpu.VMEM
    return pl.pallas_call(
        kernel,
        out_shape=jax.ShapeDtypeStruct((4, 512, 128), F32),
        in_specs=[pl.BlockSpec(memory_space=pl.ANY)] * 3,
        out_specs=pl.BlockSpec(memory_space=pltpu.VMEM),
        scratch_shapes=[
            vmem((4, 512, 512), F32), vmem((4, 512, 512), F32), vmem((4, 512, 128), F32),
            vmem((3, 1536, 512), F32), vmem((3, 1024, 128), F32),
            vmem((512, 512), F32), vmem((3, 512, 512), BF), vmem((512, 1024), F32),
            vmem((512, 128), F32), vmem((1024, 512), F32),
            vmem((8, 2, 512, 1024), BF), vmem((512, 1024), BF), vmem((8, 512, 128), F32),
            vmem((2, 512, 128), BF), vmem((1024, 128), F32), vmem((512, 128), F32),
            dma((9,)), dma((4, 3, 2)), dma((4, 3, 2)),
            dma((2, 6)), dma((2, 6)), dma((2, 2, 3)), dma((2, 2, 3)), dma((2, 12)), dma((2, 12)),
            pltpu.SemaphoreType.REGULAR((5,)),
        ],
        compiler_params=pltpu.CompilerParams(
            collective_id=0, has_side_effects=True, vmem_limit_bytes=64000 * 1024
        ),
    )(diagonal, lower, right_side)


def solution(mesh):
    in_specs = (P("seg", None, "col"), P("seg", None, None), P("seg", None, "col"))
    return jax.shard_map(
        on_device, mesh=mesh, in_specs=in_specs, out_specs=P("seg", None, "col"), check_vma=False
    )
```

```python
import functools
import jax
import jax.numpy as jnp
from jax import lax
from jax.experimental import pallas as pl
from jax.experimental.pallas import tpu as pltpu
from jax.sharding import PartitionSpec as P

W = 16
BF = jnp.bfloat16
F32 = jnp.float32


def pieces(x):
    high = x.astype(BF)
    rest = x - high.astype(F32)
    mid = rest.astype(BF)
    low = (rest - mid.astype(F32)).astype(BF)
    return high, mid, low


def beside(h, m, l):
    return jnp.concatenate([h, m, h, m, h, l], axis=1)


def below(h, m, l):
    return jnp.concatenate([h, h, m, m, l, h], axis=0)


def dot(a, b):
    return jnp.dot(a, b, preferred_element_type=F32)


def at(i, size):
    return pl.ds(pl.multiple_of(i * size, size), size)


def invert128(block):
    sub = lax.broadcasted_iota(jnp.int32, (W, 128), 0)
    lane = lax.broadcasted_iota(jnp.int32, (W, 128), 1)
    count = 128 // W
    panels = [block[W * i : W * i + W] for i in range(count)]
    for k in range(count):
        first = W * k
        rows = panels[k]
        cols = [jnp.broadcast_to(rows[:, first + p : first + p + 1], (W, 128)) for p in range(W)]
        inside = (lane >= first) & (lane < first + W)
        after = k + 1 if k + 1 < count else None
        if after is not None:
            wide = [
                jnp.broadcast_to(panels[after][:, first + p : first + p + 1], (W, 128)) for p in range(W)
            ]
        rest = [i for i in range(count) if i not in (k, after)]
        left = beside(*pieces(jnp.concatenate([panels[i] for i in rest], axis=0)))
        rows = jnp.where(inside, (lane - first == sub).astype(F32), rows)
        diag = cols[0][0:1, :]
        for p in range(W):
            pivot = 1.0 / diag
            here = sub == p
            column = cols[p]
            for j in range(p + 1, W):
                if j == p + 1:
                    moved = cols[j] - (column * cols[j][p : p + 1, :]) * pivot
                    diag = moved[j : j + 1, :]
                    cols[j] = jnp.where(here, cols[j][p : p + 1, :] * pivot, moved)
                else:
                    scaled = cols[j][p : p + 1, :] * pivot
                    cols[j] = jnp.where(here, scaled, cols[j] - column * scaled)
            scaled = rows[p : p + 1, :] * pivot
            rows = jnp.where(here, scaled, rows - column * scaled)
        if after is not None:
            acc = jnp.where(inside, 0.0, panels[after])
            for p in range(W):
                acc = acc - wide[p] * rows[p : p + 1, :]
        padded = [
            jnp.concatenate(
                [jnp.zeros((first, 128), BF)] * (first > 0)
                + [q]
                + [jnp.zeros((112 - first, 128), BF)] * (first < 112),
                axis=0,
            )
            for q in pieces(rows)
        ]
        delta = dot(left, below(*padded))
        for n, i in enumerate(rest):
            panels[i] = jnp.where(inside, 0.0, panels[i]) - delta[W * n : W * n + W]
        panels[k] = rows
        if after is not None:
            panels[after] = acc
    return jnp.concatenate(panels, axis=0)


MESH_ID = pl.DeviceIdType.MESH


def partner_of(seg, level):
    if level == 0:
        return seg + 1 - 2 * lax.rem(seg, 2)
    core, x, y = lax.rem(seg, 2), lax.rem(lax.div(seg, 2), 4), lax.div(seg, 8)
    if level == 1:
        x = x + 1 - 2 * lax.rem(x, 2)
    if level == 2:
        x = 3 - x
    if level == 3:
        y = y + 1 - 2 * lax.rem(y, 2)
    if level == 4:
        y = 3 - y
    return (y * 4 + x) * 2 + core


def invert(p, hook, started, joined):
    def step(j, late):
        s = at(j, 128)
        w = invert128(p[s, s])
        if late:
            started()
        rowid = lax.broadcasted_iota(jnp.int32, (512, 1), 0) // 128
        u6 = beside(*pieces(jnp.where(rowid == j, 0.0, p[:, s])))
        w6 = beside(*pieces(w))
        t = dot(w6, below(*pieces(p[s, :])))
        here = lax.broadcasted_iota(jnp.int32, (1, 512), 1) // 128 == j
        t = jnp.where(here, jnp.concatenate([w] * 4, axis=1), t)
        if late:
            joined()
        for n in (slice(0, 256), slice(256, 512)):
            p[:, n] = jnp.where(here[:, n], 0.0, p[:, n]) - dot(u6, below(*pieces(t[:, n])))
        p[s, :] = t

    step(0, True)

    def later(j, c):
        hook(j)
        step(j, False)
        return c

    lax.fori_loop(1, 4, later, 0)


def kernel(
    diag, low, right, x,
    dv, lv, rv, st, rh, p, p3, e, f, et, gg, gl, gf, fp, xs, keep,
    load_sem, ds, dr, xsend, xrecv, zsend, zrecv, csend, crecv, ready,
):
    seg, col = lax.axis_index("seg"), lax.axis_index("col")
    core = lax.rem(seg, 2)
    me = col * 2 + core
    sibling = (partner_of(seg, 0), col)
    around = [(seg, lax.rem(col + d, 4)) for d in (1, 2, 3)]
    across = [(partner_of(seg, level), col) for level in range(1, 5)]

    def remote(src, dst, s, d, peer):
        return pltpu.make_async_remote_copy(
            src_ref=src, dst_ref=dst, send_sem=s, recv_sem=d, device_id=peer, device_id_type=MESH_ID
        )

    columns = pl.ds(pl.multiple_of(col * 128, 128), 128)
    loads = [pltpu.make_async_copy(low.at[b], lv.at[b], load_sem.at[b]) for b in range(4)]
    loads.append(pltpu.make_async_copy(right, rv, load_sem.at[4]))
    own = [pltpu.make_async_copy(diag.at[b], dv.at[b, :, columns], load_sem.at[5 + b]) for b in range(4)]
    for c in [own[0], loads[0], loads[1], loads[4], own[2], loads[2], loads[3], own[1], own[3]]:
        c.start()
    barrier = pltpu.get_barrier_semaphore()
    for peer in [sibling] + around + across:
        pl.semaphore_signal(barrier, inc=1, device_id=peer, device_id_type=MESH_ID)
    pl.semaphore_wait(barrier, 8)
    upper = lax.div(col, 2)
    third = (1 - upper) * (3 - col) + upper * (col - 2)
    shares = [
        pl.ds(pl.multiple_of(upper * 256, 256), 256),
        pl.ds(pl.multiple_of(third * 128, 128), 128),
    ]
    slabs = [
        [
            remote(diag.at[b, r], dv.at[b, r, columns], ds.at[b, d, i], dr.at[b, d, i], around[d])
            for d in (0, 2, 1)
            for i, r in enumerate(shares)
        ]
        for b in range(4)
    ]
    for b in (0, 2, 1, 3):
        for c in slabs[b]:
            c.start()

    def arrived(b):
        own[b].wait()
        for c in slabs[b]:
            c.wait_recv()
        dv[b, 0:128, 384:512] = dv[b, 384:512, 0:128].T
        dv[b, 128:256, 256:384] = dv[b, 256:384, 128:256].T

    def node(n, power):
        other = 1 + lax.rem(n + 1, 2)
        bit = lax.rem(lax.div(seg, power), 2) * (n >= 3).astype(jnp.int32)
        a, b = bit * other, (1 - bit) * other
        par = lax.rem(n + 1, 2)

        def rows(base, i, size):
            return pl.ds(pl.multiple_of(base + i * size, size), size)

        def crossing(to, there, bit=bit, other=other, par=par):
            s, d = bit * 1024, (1 - bit) * 1024
            if there:
                s, d = d, s
            half = 512 * bit
            if there:
                half = 512 - half
            src, dst = (0, other) if there else (other, other)
            list_ = [
                (st.at[src, rows(s, core, 128)], st.at[dst, rows(s, core, 128)]),
                (st.at[src, rows(s + 256, core, 128), 256:512], st.at[dst, rows(s + 256, core, 128), 256:512]),
                (st.at[src, rows(512, me, 64)], st.at[dst, rows(512, me, 64)]),
                (st.at[src, rows(d, me, 64)], st.at[dst, rows(d, me, 64)]),
                (rh.at[src, rows(half, core, 256)], rh.at[dst, rows(half, core, 256)]),
                (rh.at[src, rows(512 - half, core, 256)], rh.at[dst, rows(512 - half, core, 256)]),
            ]
            return [remote(u, v, xsend.at[par, i], xrecv.at[par, i], to) for i, (u, v) in enumerate(list_)]

        def whole(there, bit=bit, other=other, par=par):
            s, d, half = bit * 1024, (1 - bit) * 1024, 512 * bit
            if there:
                s, d, half = d, s, 512 - half
            src = 0 if there else other
            list_ = [
                (st.at[src, rows(s, 0, 512)], st.at[other, rows(s, 0, 512)]),
                (st.at[src, rows(512, 0, 512)], st.at[other, rows(512, 0, 512)]),
                (rh.at[src, rows(half, 0, 512)], rh.at[other, rows(half, 0, 512)]),
                (st.at[src, rows(d, 0, 512)], st.at[other, rows(d, 0, 512)]),
                (rh.at[src, rows(512 - half, 0, 512)], rh.at[other, rows(512 - half, 0, 512)]),
            ]
            return [remote(u, v, xsend.at[par, i], xrecv.at[par, i], sibling) for i, (u, v) in enumerate(list_)]

        came = crossing(sibling, False)

        s_, d_, half_ = bit * 1024, (1 - bit) * 1024, 512 * bit
        got = [
            st.at[other, rows(s_, core, 128)],
            st.at[other, rows(s_ + 256, core, 128), 256:512],
            st.at[other, rows(512, me, 64)],
            st.at[other, rows(d_, me, 64)],
            rh.at[other, rows(half_, core, 256)],
            rh.at[other, rows(512 - half_, core, 256)],
        ]

        def to_sibling(i, ref):
            return remote(ref, ref, csend.at[par, i], crecv.at[par, i], sibling)

        def round_z(kind):
            i = 2 + kind
            return [
                remote(got[i], got[i], zsend.at[par, kind, d], zrecv.at[par, kind, d], around[d])
                for d in range(3)
            ]

        def from_z(kind):
            base = 512 if kind == 0 else d_
            out = []
            for d in range(3):
                owner = lax.rem(col + 3 - d, 4) * 2 + core
                ref = st.at[other, rows(base, owner, 64)]
                out.append(to_sibling(6 + 3 * kind + d, ref))
            return out

        direct = [to_sibling(i, got[i]) for i in range(6)]
        far = n >= 4

        def hook(j):
            for kind in (0, 1):

                @pl.when(far & (n < 8) & (j == 1 + kind))
                def _(kind=kind):
                    came[2 + kind].wait_recv()
                    for c in round_z(kind):
                        c.start()
                    direct[2 + kind].start()

        def started():
            @pl.when(far & (n < 8))
            def _():
                came[1].wait_recv()
                direct[1].start()

        def joined():
            @pl.when(far & (n < 8))
            def _():
                direct[1].wait_recv()
                p[256:512, 256:512] = st[a, 1280:1536, 256:512] + st[b, 256:512, 256:512]

        def left_couplings(source):
            et[0:512, :] = source
            e[:, 0:512] = source.T

        def right_couplings(source):
            e[:, 512:1024] = source
            et[512:1024, :] = source.T

        merging = (n >= 2) & (n < 8)

        @pl.when(n == 0)
        def _():
            loads[0].wait()
            loads[1].wait()
            loads[4].wait()

        @pl.when(n == 1)
        def _():
            loads[2].wait()
            loads[3].wait()

        @pl.when(n < 2)
        def _():
            q = 2 * n
            has_left = 1.0 - ((n == 0) & (seg == 0)).astype(F32)
            et[512:1024, :] = lv[q + 1]
            e[:, 0:512] = lv[q] * has_left
            et[0:512, :] = e[:, 0:512].T
            e[:, 512:1024] = et[512:1024, :].T
            f[...] = rv[q]
            st[q] = jnp.zeros((1536, 512), F32)
            rh[q] = jnp.zeros((1024, 128), F32)

        @pl.when(n == 0)
        def _():
            arrived(0)
            p[...] = dv[0]

        @pl.when(n == 1)
        def _():
            arrived(2)
            p[...] = dv[2]

        @pl.when(n == 2)
        def _():
            arrived(1)
            arrived(3)

        @pl.when(n == 3)
        def _():
            whole(False)[0].wait_recv()

        @pl.when(merging & (bit == 0))
        def _():
            left_couplings(st[0, 512:1024, :])

        @pl.when(merging & (bit == 1))
        def _():
            right_couplings(st[0, 512:1024, :])

        @pl.when(far & (n < 8))
        def _():
            came[0].wait_recv()
            direct[0].start()
            direct[0].wait_recv()
            p[0:256, :] = st[a, 1024:1280, :] + st[b, 0:256, :]

        @pl.when((n == 2) | (n == 3))
        def _():
            p[...] = st[a, 1024:1536, :] + st[b, 0:512, :]

        @pl.when(n == 2)
        def _():
            p[...] = p[...] + dv[1]

        @pl.when(n == 8)
        def _():
            p[...] = st[0, 1024:1536, :]

        p[256:512, 0:256] = p[0:256, 256:512].T
        invert(p, hook, started, joined)

        @pl.when(n < 8)
        def _():
            for q, part in enumerate(pieces(p[...])):
                p3[q] = part

            @pl.when(far)
            def _():
                came[4].wait_recv()
                direct[4].start()
                for c, onward in zip(round_z(0), from_z(0)):
                    c.wait_recv()
                    onward.start()

            def tile(i, c):
                k = at(lax.rem(i + 2 * bit, 4), 256)
                out = dot(beside(p3[0], p3[1], p3[2]), below(*pieces(e[:, k])))
                gg[n, 0, :, k], gg[n, 1, :, k], gl[:, k] = pieces(out)
                return c

            def half_of(i, c):
                @pl.when((i == 1) & (n == 3))
                def _():
                    for c in whole(False)[1:]:
                        c.wait_recv()

                @pl.when((i == 1) & far)
                def _():
                    for c in [direct[2], direct[4]] + from_z(0):
                        c.wait_recv()
                    came[5].wait_recv()
                    direct[5].start()

                @pl.when((i == 1) & merging & (bit == 0))
                def _():
                    right_couplings(st[other, 512:1024, :])

                @pl.when((i == 1) & merging & (bit == 1))
                def _():
                    left_couplings(st[other, 512:1024, :])

                lax.fori_loop(2 * i, 2 * i + 2, tile, 0)
                return c

            lax.fori_loop(0, 2, half_of, 0)

            @pl.when(far)
            def _():
                for c, onward in zip(round_z(1), from_z(1)):
                    c.wait_recv()
                    onward.start()

            @pl.when(n >= 2)
            def _():
                f[...] = rh[a, 512:1024, :] + rh[b, 0:512, :]

            @pl.when(n == 2)
            def _():
                f[...] = f[...] + rv[1]

            fh, fm, _ = pieces(f[...])
            out = dot(
                jnp.concatenate([p3[0], p3[1], p3[0]], axis=1), jnp.concatenate([fh, fh, fm], axis=0)
            )
            gf[n] = out
            fp[0], fp[1], _ = pieces(out)

            @pl.when(n == 3)
            def _():
                for c in whole(True):
                    c.wait_send()

            @pl.when(far)
            def _():
                for c in [direct[3], direct[5]] + from_z(1):
                    c.wait_recv()
                for c in crossing(sibling, True) + direct + round_z(0) + round_z(1) + from_z(0) + from_z(1):
                    c.wait_send()

            @pl.when(n >= 2)
            def _():
                r = pl.ds(pl.multiple_of((1 - bit) * 1024, 512), 512)
                st[0, r, :] = st[other, r, :]
                r = pl.ds(pl.multiple_of((1 - bit) * 512, 512), 512)
                rh[0, r, :] = rh[other, r, :]

            @pl.when(n == 2)
            def _():
                st[0, 1024:1536, :] = st[0, 1024:1536, :] + dv[3]
                rh[0, 512:1024, :] = rh[0, 512:1024, :] + rv[3]

            t = 2 * (n == 1).astype(jnp.int32)

            def term(i, k):
                k = at(k, 256)
                return dot(beside(*pieces(et[at(i, 256), :])), below(gg[n, 0, :, k], gg[n, 1, :, k], gl[:, k]))

            following = power * (1 + (n >= 3).astype(jnp.int32))
            sends = (n >= 2) & (n < 7)
            turn = lax.rem(lax.div(seg, following), 2)
            first = 1 - turn * sends.astype(jnp.int32)
            to = dict(bit=turn, other=1 + lax.rem(n, 2), par=lax.rem(n, 2))

            def send(part):
                @pl.when(n == 2)
                def _():
                    for c in whole(True, **to)[:1] if part == 0 else whole(True, **to)[1:]:
                        c.start()

                for level in range(1, 5):

                    @pl.when(n == 2 + level)
                    def _(level=level):
                        out = crossing(across[level - 1], True, **to)
                        if part == 0:
                            pl.semaphore_wait(ready.at[level], 5)
                        for c in out[:2] if part == 0 else out[2:]:
                            c.start()

            def corners(turned, c):
                w = first + turned * (1 - 2 * first)

                def corner(q, c):
                    i, k = q // 2 + 4 * w, (q + 1) // 2
                    r = at(i, 256)
                    st[t, r, at(k, 256)] = st[t, r, at(k, 256)] - term(q // 2 + 2 * w, k + 2 * w)
                    return c

                lax.fori_loop(0, 3, corner, 0)
                st[t, at(4 * w + 1, 256), 0:256] = st[t, at(4 * w, 256), 256:512].T
                pl.when(turned == 0)(lambda: send(0))
                return c

            lax.fori_loop(0, 2 - (n == 7).astype(jnp.int32), corners, 0)

            @pl.when(n < 7)
            def _():
                def square(q, c):
                    i, k = q // 2, q % 2
                    st[t, at(i + 2, 256), at(k, 256)] = -term(i, k + 2)
                    return c

                lax.fori_loop(0, 4, square, 0)

            def side(i, c):
                r = at(i, 256)
                h, m, _ = pieces(et[r, :])
                rh[t, r, :] = rh[t, r, :] - dot(
                    jnp.concatenate([h, m, h], axis=1), jnp.concatenate([fp[0], fp[0], fp[1]], axis=0)
                )
                return c

            lax.fori_loop(0, 4, side, 0)
            send(1)
            for level in range(1, 5):

                @pl.when(n == level + 1)
                def _(level=level):
                    for peer in [sibling, across[level - 1]] + around:
                        pl.semaphore_signal(
                            ready.at[level], inc=1, device_id=peer, device_id_type=MESH_ID
                        )

        return power * (1 + (n >= 3).astype(jnp.int32))

    lax.fori_loop(0, 9, node, jnp.int32(1))
    for b in range(4):
        for c in slabs[b]:
            c.wait_send()
    xs[0:512, :] = jnp.zeros((512, 128), F32)
    last = dot(beside(*pieces(p[...])), below(*pieces(rh[0, 512:1024, :])))
    xs[512:1024, :] = last
    x[3] = jnp.zeros((512, 128), F32)

    def back(i, power):
        n = 7 - i
        h, m, _ = pieces(xs[...])
        middle = gf[n] - dot(
            jnp.concatenate([gg[n, 0], gg[n, 1], gg[n, 0]], axis=1), jnp.concatenate([h, h, m], axis=0)
        )

        @pl.when(n >= 3)
        def _():
            bit = lax.rem(lax.div(seg, power), 2)
            xs[pl.ds(pl.multiple_of((1 - bit) * 512, 512), 512), :] = middle

        @pl.when(n == 2)
        def _():
            x[3] = xs[512:1024, :]
            x[1] = middle
            keep[...] = xs[0:512, :]
            xs[0:512, :] = middle

        @pl.when(n == 1)
        def _():
            x[2] = middle
            xs[512:1024, :] = xs[0:512, :]
            xs[0:512, :] = keep[...]

        @pl.when(n == 0)
        def _():
            x[0] = middle

        return power // (1 + (n > 3).astype(jnp.int32))

    lax.fori_loop(0, 8, back, jnp.int32(16))


def on_device(diagonal, lower, right_side):
    dma = pltpu.SemaphoreType.DMA
    vmem = pltpu.VMEM
    return pl.pallas_call(
        kernel,
        out_shape=jax.ShapeDtypeStruct((4, 512, 128), F32),
        in_specs=[pl.BlockSpec(memory_space=pl.ANY)] * 3,
        out_specs=pl.BlockSpec(memory_space=pltpu.VMEM),
        scratch_shapes=[
            vmem((4, 512, 512), F32), vmem((4, 512, 512), F32), vmem((4, 512, 128), F32),
            vmem((3, 1536, 512), F32), vmem((3, 1024, 128), F32),
            vmem((512, 512), F32), vmem((3, 512, 512), BF), vmem((512, 1024), F32),
            vmem((512, 128), F32), vmem((1024, 512), F32),
            vmem((8, 2, 512, 1024), BF), vmem((512, 1024), BF), vmem((8, 512, 128), F32),
            vmem((2, 512, 128), BF), vmem((1024, 128), F32), vmem((512, 128), F32),
            dma((9,)), dma((4, 3, 2)), dma((4, 3, 2)),
            dma((2, 6)), dma((2, 6)), dma((2, 2, 3)), dma((2, 2, 3)), dma((2, 12)), dma((2, 12)),
            pltpu.SemaphoreType.REGULAR((5,)),
        ],
        compiler_params=pltpu.CompilerParams(
            collective_id=0, has_side_effects=True, vmem_limit_bytes=64000 * 1024
        ),
    )(diagonal, lower, right_side)


def solution(mesh):
    in_specs = (P("seg", None, "col"), P("seg", None, None), P("seg", None, "col"))
    return jax.shard_map(
        on_device, mesh=mesh, in_specs=in_specs, out_specs=P("seg", None, "col"), check_vma=False
    )
```

```python
import functools
import jax
import jax.numpy as jnp
from jax import lax
from jax.experimental import pallas as pl
from jax.experimental.pallas import tpu as pltpu
from jax.sharding import PartitionSpec as P

W = 16
BF = jnp.bfloat16
F32 = jnp.float32


def pieces(x):
    high = x.astype(BF)
    rest = x - high.astype(F32)
    mid = rest.astype(BF)
    low = (rest - mid.astype(F32)).astype(BF)
    return high, mid, low


def beside(h, m, l):
    return jnp.concatenate([h, m, h, m, h, l], axis=1)


def below(h, m, l):
    return jnp.concatenate([h, h, m, m, l, h], axis=0)


def dot(a, b):
    return jnp.dot(a, b, preferred_element_type=F32)


def at(i, size):
    return pl.ds(pl.multiple_of(i * size, size), size)


def invert128(block):
    sub = lax.broadcasted_iota(jnp.int32, (W, 128), 0)
    lane = lax.broadcasted_iota(jnp.int32, (W, 128), 1)
    count = 128 // W
    panels = [block[W * i : W * i + W] for i in range(count)]
    for k in range(count):
        first = W * k
        rows = panels[k]
        near = [i for i in (k + 1,) if i < count]
        cols, wide = [], {i: [] for i in near}
        for p in range(W):
            cols.append(jnp.broadcast_to(rows[:, first + p : first + p + 1], (W, 128)))
        for i in near:
            for p in range(W):
                wide[i].append(jnp.broadcast_to(panels[i][:, first + p : first + p + 1], (W, 128)))
        inside = (lane >= first) & (lane < first + W)
        rest = [i for i in range(count) if i != k and i not in near]
        if rest:
            left = beside(*pieces(jnp.concatenate([panels[i] for i in rest], axis=0)))
        rows = jnp.where(inside, (lane - first == sub).astype(F32), rows)
        diag = cols[0][0:1, :]
        for p in range(W):
            pivot = 1.0 / diag
            here = sub == p
            column = cols[p]
            for j in range(p + 1, W):
                scaled = cols[j][p : p + 1, :] * pivot
                moved = cols[j] - column * scaled
                if j == p + 1:
                    diag = moved[j : j + 1, :]
                cols[j] = jnp.where(here, scaled, moved)
            scaled = rows[p : p + 1, :] * pivot
            rows = jnp.where(here, scaled, rows - column * scaled)
        if rest:
            padded = [
                jnp.concatenate(
                    [jnp.zeros((first, 128), BF)] * (first > 0)
                    + [q]
                    + [jnp.zeros((112 - first, 128), BF)] * (first < 112),
                    axis=0,
                )
                for q in pieces(rows)
            ]
            delta = dot(left, below(*padded))
            for n, i in enumerate(rest):
                panels[i] = jnp.where(inside, 0.0, panels[i]) - delta[W * n : W * n + W]
        for i in near:
            sums = [wide[i][p] * rows[p : p + 1, :] for p in range(4)]
            for p in range(4, W):
                sums[p % 4] = sums[p % 4] + wide[i][p] * rows[p : p + 1, :]
            panels[i] = jnp.where(inside, 0.0, panels[i]) - ((sums[0] + sums[1]) + (sums[2] + sums[3]))
        panels[k] = rows
    return jnp.concatenate(panels, axis=0)


MESH_ID = pl.DeviceIdType.MESH


def partner_of(seg, level):
    if level == 0:
        return seg + 1 - 2 * lax.rem(seg, 2)
    core, x, y = lax.rem(seg, 2), lax.rem(lax.div(seg, 2), 4), lax.div(seg, 8)
    if level == 1:
        x = x + 1 - 2 * lax.rem(x, 2)
    if level == 2:
        x = 3 - x
    if level == 3:
        y = y + 1 - 2 * lax.rem(y, 2)
    if level == 4:
        y = 3 - y
    return (y * 4 + x) * 2 + core


def invert(p, hook, started, joined):
    def step(j, late):
        s = at(j, 128)
        w = invert128(p[s, s])
        if late:
            started()
        rowid = lax.broadcasted_iota(jnp.int32, (512, 1), 0) // 128
        u6 = beside(*pieces(jnp.where(rowid == j, 0.0, p[:, s])))
        w6 = beside(*pieces(w))
        t = dot(w6, below(*pieces(p[s, :])))
        here = lax.broadcasted_iota(jnp.int32, (1, 512), 1) // 128 == j
        t = jnp.where(here, jnp.concatenate([w] * 4, axis=1), t)
        if late:
            joined()
        for n in (slice(0, 256), slice(256, 512)):
            p[:, n] = jnp.where(here[:, n], 0.0, p[:, n]) - dot(u6, below(*pieces(t[:, n])))
        p[s, :] = t

    step(0, True)

    def later(j, c):
        hook(j)
        step(j, False)
        return c

    lax.fori_loop(1, 4, later, 0)


def kernel(
    diag, low, right, x,
    dv, lv, rv, st, rh, p, p3, e, f, et, gg, gl, gf, fp, xs, keep,
    load_sem, ds, dr, xsend, xrecv, zsend, zrecv, csend, crecv, ready,
):
    seg, col = lax.axis_index("seg"), lax.axis_index("col")
    core = lax.rem(seg, 2)
    me = col * 2 + core
    sibling = (partner_of(seg, 0), col)
    around = [(seg, lax.rem(col + d, 4)) for d in (1, 2, 3)]
    across = [(partner_of(seg, level), col) for level in range(1, 5)]

    def remote(src, dst, s, d, peer):
        return pltpu.make_async_remote_copy(
            src_ref=src, dst_ref=dst, send_sem=s, recv_sem=d, device_id=peer, device_id_type=MESH_ID
        )

    columns = pl.ds(pl.multiple_of(col * 128, 128), 128)
    loads = [pltpu.make_async_copy(low.at[b], lv.at[b], load_sem.at[b]) for b in range(4)]
    loads.append(pltpu.make_async_copy(right, rv, load_sem.at[4]))
    own = [pltpu.make_async_copy(diag.at[b], dv.at[b, :, columns], load_sem.at[5 + b]) for b in range(4)]
    for c in [own[0], loads[0], loads[1], loads[4], own[2], loads[2], loads[3], own[1], own[3]]:
        c.start()
    barrier = pltpu.get_barrier_semaphore()
    for peer in [sibling] + around + across:
        pl.semaphore_signal(barrier, inc=1, device_id=peer, device_id_type=MESH_ID)
    pl.semaphore_wait(barrier, 8)
    upper = lax.div(col, 2)
    third = (1 - upper) * (3 - col) + upper * (col - 2)
    shares = [
        pl.ds(pl.multiple_of(upper * 256, 256), 256),
        pl.ds(pl.multiple_of(third * 128, 128), 128),
    ]
    slabs = [
        [
            remote(diag.at[b, r], dv.at[b, r, columns], ds.at[b, d, i], dr.at[b, d, i], around[d])
            for d in (0, 2, 1)
            for i, r in enumerate(shares)
        ]
        for b in range(4)
    ]
    for b in (0, 2, 1, 3):
        for c in slabs[b]:
            c.start()

    def arrived(b):
        own[b].wait()
        for c in slabs[b]:
            c.wait_recv()
        dv[b, 0:128, 384:512] = dv[b, 384:512, 0:128].T
        dv[b, 128:256, 256:384] = dv[b, 256:384, 128:256].T

    def node(n, power):
        other = 1 + lax.rem(n + 1, 2)
        bit = lax.rem(lax.div(seg, power), 2) * (n >= 3).astype(jnp.int32)
        a, b = bit * other, (1 - bit) * other
        par = lax.rem(n + 1, 2)

        def rows(base, i, size):
            return pl.ds(pl.multiple_of(base + i * size, size), size)

        def crossing(to, there, bit=bit, other=other, par=par):
            s, d = bit * 1024, (1 - bit) * 1024
            if there:
                s, d = d, s
            half = 512 * bit
            if there:
                half = 512 - half
            src, dst = (0, other) if there else (other, other)
            list_ = [
                (st.at[src, rows(s, core, 128)], st.at[dst, rows(s, core, 128)]),
                (st.at[src, rows(s + 256, core, 128), 256:512], st.at[dst, rows(s + 256, core, 128), 256:512]),
                (st.at[src, rows(512, me, 64)], st.at[dst, rows(512, me, 64)]),
                (st.at[src, rows(d, me, 64)], st.at[dst, rows(d, me, 64)]),
                (rh.at[src, rows(half, core, 256)], rh.at[dst, rows(half, core, 256)]),
                (rh.at[src, rows(512 - half, core, 256)], rh.at[dst, rows(512 - half, core, 256)]),
            ]
            return [remote(u, v, xsend.at[par, i], xrecv.at[par, i], to) for i, (u, v) in enumerate(list_)]

        def whole(there, bit=bit, other=other, par=par):
            s, d, half = bit * 1024, (1 - bit) * 1024, 512 * bit
            if there:
                s, d, half = d, s, 512 - half
            src = 0 if there else other
            list_ = [
                (st.at[src, rows(s, 0, 512)], st.at[other, rows(s, 0, 512)]),
                (st.at[src, rows(512, 0, 512)], st.at[other, rows(512, 0, 512)]),
                (rh.at[src, rows(half, 0, 512)], rh.at[other, rows(half, 0, 512)]),
                (st.at[src, rows(d, 0, 512)], st.at[other, rows(d, 0, 512)]),
                (rh.at[src, rows(512 - half, 0, 512)], rh.at[other, rows(512 - half, 0, 512)]),
            ]
            return [remote(u, v, xsend.at[par, i], xrecv.at[par, i], sibling) for i, (u, v) in enumerate(list_)]

        came = crossing(sibling, False)

        s_, d_, half_ = bit * 1024, (1 - bit) * 1024, 512 * bit
        got = [
            st.at[other, rows(s_, core, 128)],
            st.at[other, rows(s_ + 256, core, 128), 256:512],
            st.at[other, rows(512, me, 64)],
            st.at[other, rows(d_, me, 64)],
            rh.at[other, rows(half_, core, 256)],
            rh.at[other, rows(512 - half_, core, 256)],
        ]

        def to_sibling(i, ref):
            return remote(ref, ref, csend.at[par, i], crecv.at[par, i], sibling)

        def round_z(kind):
            i = 2 + kind
            return [
                remote(got[i], got[i], zsend.at[par, kind, d], zrecv.at[par, kind, d], around[d])
                for d in range(3)
            ]

        def from_z(kind):
            base = 512 if kind == 0 else d_
            out = []
            for d in range(3):
                owner = lax.rem(col + 3 - d, 4) * 2 + core
                ref = st.at[other, rows(base, owner, 64)]
                out.append(to_sibling(6 + 3 * kind + d, ref))
            return out

        direct = [to_sibling(i, got[i]) for i in range(6)]
        far = n >= 4

        def hook(j):
            for kind in (0, 1):

                @pl.when(far & (n < 8) & (j == 1 + kind))
                def _(kind=kind):
                    came[2 + kind].wait_recv()
                    for c in round_z(kind):
                        c.start()
                    direct[2 + kind].start()

        def started():
            @pl.when(far & (n < 8))
            def _():
                came[1].wait_recv()
                direct[1].start()

        def joined():
            @pl.when(far & (n < 8))
            def _():
                direct[1].wait_recv()
                p[256:512, 256:512] = st[a, 1280:1536, 256:512] + st[b, 256:512, 256:512]

        def left_couplings(source):
            et[0:512, :] = source
            e[:, 0:512] = source.T

        def right_couplings(source):
            e[:, 512:1024] = source
            et[512:1024, :] = source.T

        merging = (n >= 2) & (n < 8)

        @pl.when(n == 0)
        def _():
            loads[0].wait()
            loads[1].wait()
            loads[4].wait()

        @pl.when(n == 1)
        def _():
            loads[2].wait()
            loads[3].wait()

        @pl.when(n < 2)
        def _():
            q = 2 * n
            has_left = 1.0 - ((n == 0) & (seg == 0)).astype(F32)
            et[512:1024, :] = lv[q + 1]
            e[:, 0:512] = lv[q] * has_left
            et[0:512, :] = e[:, 0:512].T
            e[:, 512:1024] = et[512:1024, :].T
            f[...] = rv[q]
            st[q] = jnp.zeros((1536, 512), F32)
            rh[q] = jnp.zeros((1024, 128), F32)

        @pl.when(n == 0)
        def _():
            arrived(0)
            p[...] = dv[0]

        @pl.when(n == 1)
        def _():
            arrived(2)
            p[...] = dv[2]

        @pl.when(n == 2)
        def _():
            arrived(1)
            arrived(3)

        @pl.when(n == 3)
        def _():
            whole(False)[0].wait_recv()

        @pl.when(merging & (bit == 0))
        def _():
            left_couplings(st[0, 512:1024, :])

        @pl.when(merging & (bit == 1))
        def _():
            right_couplings(st[0, 512:1024, :])

        @pl.when(far & (n < 8))
        def _():
            came[0].wait_recv()
            direct[0].start()
            direct[0].wait_recv()
            p[0:256, :] = st[a, 1024:1280, :] + st[b, 0:256, :]

        @pl.when((n == 2) | (n == 3))
        def _():
            p[...] = st[a, 1024:1536, :] + st[b, 0:512, :]

        @pl.when(n == 2)
        def _():
            p[...] = p[...] + dv[1]

        @pl.when(n == 8)
        def _():
            p[...] = st[0, 1024:1536, :]

        p[256:512, 0:256] = p[0:256, 256:512].T
        invert(p, hook, started, joined)

        @pl.when(n < 8)
        def _():
            for q, part in enumerate(pieces(p[...])):
                p3[q] = part

            @pl.when(far)
            def _():
                came[4].wait_recv()
                direct[4].start()
                for c, onward in zip(round_z(0), from_z(0)):
                    c.wait_recv()
                    onward.start()

            def tile(i, c):
                k = at(lax.rem(i + 2 * bit, 4), 256)
                out = dot(beside(p3[0], p3[1], p3[2]), below(*pieces(e[:, k])))
                gg[n, 0, :, k], gg[n, 1, :, k], gl[:, k] = pieces(out)
                return c

            def half_of(i, c):
                @pl.when((i == 1) & (n == 3))
                def _():
                    for c in whole(False)[1:]:
                        c.wait_recv()

                @pl.when((i == 1) & far)
                def _():
                    for c in [direct[2], direct[4]] + from_z(0):
                        c.wait_recv()
                    came[5].wait_recv()
                    direct[5].start()

                @pl.when((i == 1) & merging & (bit == 0))
                def _():
                    right_couplings(st[other, 512:1024, :])

                @pl.when((i == 1) & merging & (bit == 1))
                def _():
                    left_couplings(st[other, 512:1024, :])

                tile(2 * i, 0)
                tile(2 * i + 1, 0)
                return c

            lax.fori_loop(0, 2, half_of, 0)

            @pl.when(far)
            def _():
                for c, onward in zip(round_z(1), from_z(1)):
                    c.wait_recv()
                    onward.start()

            @pl.when(n >= 2)
            def _():
                f[...] = rh[a, 512:1024, :] + rh[b, 0:512, :]

            @pl.when(n == 2)
            def _():
                f[...] = f[...] + rv[1]

            fh, fm, _ = pieces(f[...])
            out = dot(
                jnp.concatenate([p3[0], p3[1], p3[0]], axis=1), jnp.concatenate([fh, fh, fm], axis=0)
            )
            gf[n] = out
            fp[0], fp[1], _ = pieces(out)

            @pl.when(n == 3)
            def _():
                for c in whole(True):
                    c.wait_send()

            @pl.when(far)
            def _():
                for c in [direct[3], direct[5]] + from_z(1):
                    c.wait_recv()
                for c in crossing(sibling, True) + direct + round_z(0) + round_z(1) + from_z(0) + from_z(1):
                    c.wait_send()

            @pl.when(n >= 2)
            def _():
                r = pl.ds(pl.multiple_of((1 - bit) * 1024, 512), 512)
                st[0, r, :] = st[other, r, :]
                r = pl.ds(pl.multiple_of((1 - bit) * 512, 512), 512)
                rh[0, r, :] = rh[other, r, :]

            @pl.when(n == 2)
            def _():
                st[0, 1024:1536, :] = st[0, 1024:1536, :] + dv[3]
                rh[0, 512:1024, :] = rh[0, 512:1024, :] + rv[3]

            t = 2 * (n == 1).astype(jnp.int32)

            def term(i, k):
                k = at(k, 256)
                return dot(beside(*pieces(et[at(i, 256), :])), below(gg[n, 0, :, k], gg[n, 1, :, k], gl[:, k]))

            following = power * (1 + (n >= 3).astype(jnp.int32))
            sends = (n >= 2) & (n < 7)
            turn = lax.rem(lax.div(seg, following), 2)
            first = 1 - turn * sends.astype(jnp.int32)
            to = dict(bit=turn, other=1 + lax.rem(n, 2), par=lax.rem(n, 2))

            def send(part):
                @pl.when(n == 2)
                def _():
                    for c in whole(True, **to)[:1] if part == 0 else whole(True, **to)[1:]:
                        c.start()

                for level in range(1, 5):

                    @pl.when(n == 2 + level)
                    def _(level=level):
                        out = crossing(across[level - 1], True, **to)
                        if part == 0:
                            pl.semaphore_wait(ready.at[level], 5)
                        for c in out[:2] if part == 0 else out[2:]:
                            c.start()

            def corners(turned, c):
                w = first + turned * (1 - 2 * first)

                def corner(q, c):
                    i, k = q // 2 + 4 * w, (q + 1) // 2
                    r = at(i, 256)
                    st[t, r, at(k, 256)] = st[t, r, at(k, 256)] - term(q // 2 + 2 * w, k + 2 * w)
                    return c

                for q in range(3):
                    corner(q, 0)
                st[t, at(4 * w + 1, 256), 0:256] = st[t, at(4 * w, 256), 256:512].T
                pl.when(turned == 0)(lambda: send(0))
                return c

            lax.fori_loop(0, 2 - (n == 7).astype(jnp.int32), corners, 0)

            @pl.when(n < 7)
            def _():
                def square(q, c):
                    i, k = q // 2, q % 2
                    st[t, at(i + 2, 256), at(k, 256)] = -term(i, k + 2)
                    return c

                lax.fori_loop(0, 4, square, 0, unroll=4)

            def side(i, c):
                r = at(i, 256)
                h, m, _ = pieces(et[r, :])
                rh[t, r, :] = rh[t, r, :] - dot(
                    jnp.concatenate([h, m, h], axis=1), jnp.concatenate([fp[0], fp[0], fp[1]], axis=0)
                )
                return c

            lax.fori_loop(0, 4, side, 0, unroll=4)
            send(1)
            for level in range(1, 5):

                @pl.when(n == level + 1)
                def _(level=level):
                    for peer in [sibling, across[level - 1]] + around:
                        pl.semaphore_signal(
                            ready.at[level], inc=1, device_id=peer, device_id_type=MESH_ID
                        )

        return power * (1 + (n >= 3).astype(jnp.int32))

    lax.fori_loop(0, 9, node, jnp.int32(1))
    for b in range(4):
        for c in slabs[b]:
            c.wait_send()
    xs[0:512, :] = jnp.zeros((512, 128), F32)
    last = dot(beside(*pieces(p[...])), below(*pieces(rh[0, 512:1024, :])))
    xs[512:1024, :] = last
    x[3] = jnp.zeros((512, 128), F32)

    def back(i, power):
        n = 7 - i
        h, m, _ = pieces(xs[...])
        middle = gf[n] - dot(
            jnp.concatenate([gg[n, 0], gg[n, 1], gg[n, 0]], axis=1), jnp.concatenate([h, h, m], axis=0)
        )

        @pl.when(n >= 3)
        def _():
            bit = lax.rem(lax.div(seg, power), 2)
            xs[pl.ds(pl.multiple_of((1 - bit) * 512, 512), 512), :] = middle

        @pl.when(n == 2)
        def _():
            x[3] = xs[512:1024, :]
            x[1] = middle
            keep[...] = xs[0:512, :]
            xs[0:512, :] = middle

        @pl.when(n == 1)
        def _():
            x[2] = middle
            xs[512:1024, :] = xs[0:512, :]
            xs[0:512, :] = keep[...]

        @pl.when(n == 0)
        def _():
            x[0] = middle

        return power // (1 + (n > 3).astype(jnp.int32))

    lax.fori_loop(0, 8, back, jnp.int32(16))


def on_device(diagonal, lower, right_side):
    dma = pltpu.SemaphoreType.DMA
    vmem = pltpu.VMEM
    return pl.pallas_call(
        kernel,
        out_shape=jax.ShapeDtypeStruct((4, 512, 128), F32),
        in_specs=[pl.BlockSpec(memory_space=pl.ANY)] * 3,
        out_specs=pl.BlockSpec(memory_space=pltpu.VMEM),
        scratch_shapes=[
            vmem((4, 512, 512), F32), vmem((4, 512, 512), F32), vmem((4, 512, 128), F32),
            vmem((3, 1536, 512), F32), vmem((3, 1024, 128), F32),
            vmem((512, 512), F32), vmem((3, 512, 512), BF), vmem((512, 1024), F32),
            vmem((512, 128), F32), vmem((1024, 512), F32),
            vmem((8, 2, 512, 1024), BF), vmem((512, 1024), BF), vmem((8, 512, 128), F32),
            vmem((2, 512, 128), BF), vmem((1024, 128), F32), vmem((512, 128), F32),
            dma((9,)), dma((4, 3, 2)), dma((4, 3, 2)),
            dma((2, 6)), dma((2, 6)), dma((2, 2, 3)), dma((2, 2, 3)), dma((2, 12)), dma((2, 12)),
            pltpu.SemaphoreType.REGULAR((5,)),
        ],
        compiler_params=pltpu.CompilerParams(
            collective_id=0, has_side_effects=True, vmem_limit_bytes=64000 * 1024
        ),
    )(diagonal, lower, right_side)


def solution(mesh):
    in_specs = (P("seg", None, "col"), P("seg", None, None), P("seg", None, "col"))
    return jax.shard_map(
        on_device, mesh=mesh, in_specs=in_specs, out_specs=P("seg", None, "col"), check_vma=False
    )
```
